1024 devices in a mesh: segment: 16 (over z), tok: 32 (over x, y), mp: 2 (over core).
Axes of the slice: x: 4, y: 8, z: 16, core: 2. Of those that a mesh axis runs over, the one named last changes fastest.
Arguments:
- out_cotangent: bfloat16 [16, 4096, 4096], P('segment', 'tok', 'mp'), may hold values from -6 to 6
- block_output: bfloat16 [16, 4096, 4096], P('segment', 'tok', 'mp'), may hold values from -6 to 6
- router_logits: float32 [16, 4096], P('segment', 'tok'), may hold values from -8 to 8
- keep_flags: int32 [16, 4096], P('segment', 'tok'), may hold values from 0 to 1, as said below
- router_weight: float32 [16, 4096], P('segment', 'mp'), may hold values from -0.09375 to 0.09375
- activated: bfloat16 [16, 512, 14336], P('segment', None, 'tok'), may hold values from -4 to 4
Outputs:
- cotangent_received: bfloat16 [16, 4096, 4096], P('segment', 'tok', 'mp')
- grad_out: bfloat16 [16, 4096, 14336], P('segment', 'mp', 'tok')
The draws below stay inside these ranges and needn't reach their ends.
Inputs may be any that keep to these rules, and one draw needn't show every extreme that they name: `keep_flags`: in every segment each aligned block of 128 tokens (one device of a group) holds at most 48 active tokens, some block holds exactly 48, and the segment holds exactly 512 active tokens.
All inputs are finite; a program needn't handle non-finite values.
Results may differ from the reference program's by a relative error of at most 0.0049.
Values may be sent and summed in bfloat16 or wider, within the bound.
A program may use at most 32 MiB of HBM per device.

```python
import jax
import jax.numpy as jnp
from jax import lax

D = 4096
HID = 14336
TOK_DEV = 128
TOKENS = 4096
GROUP_ACTIVE = 512
RELAY_SECTIONS = 16


def draw_keep_flags(key, part):
    token_groups = TOKENS // TOK_DEV
    average = TOK_DEV // 8
    largest_row_count = 3 * average
    key_weight = jax.random.fold_in(key, 11)
    key_heavy = jax.random.fold_in(key, 12)
    key_extra = jax.random.fold_in(key, 13)
    key_place = jax.random.fold_in(key, 14)
    weights = jax.random.randint(key_weight, (RELAY_SECTIONS, token_groups), 2, 5)
    heaviest = jax.random.randint(key_heavy, (RELAY_SECTIONS, 1), 0, token_groups)
    device_index = jnp.arange(token_groups, dtype=jnp.int32)[None, :]
    heavy_flag = device_index == heaviest
    weights = jnp.where(heavy_flag, 0, weights)
    remainder = token_groups * average - largest_row_count
    weight_sum = jnp.sum(weights, axis=1, keepdims=True)
    row_shares = remainder * weights // weight_sum
    spare_rows = remainder - jnp.sum(row_shares, axis=1, keepdims=True)
    within_remaining = device_index - (device_index > heaviest).astype(jnp.int32)
    cyclic_shift = jax.random.randint(key_extra, (RELAY_SECTIONS, 1), 0, token_groups - 1)
    extra_row = (jnp.mod(within_remaining + cyclic_shift, token_groups - 1) < spare_rows).astype(jnp.int32)
    row_count_list = jnp.where(heavy_flag, largest_row_count, row_shares + extra_row)
    row_keys = jax.random.split(key_place, RELAY_SECTIONS * token_groups)
    token_rank = jax.vmap(lambda one_key: jax.random.permutation(one_key, TOK_DEV))(row_keys)
    token_rank = token_rank.reshape(RELAY_SECTIONS, token_groups, TOK_DEV)
    keep_flags = (token_rank < row_count_list[:, :, None]).astype(jnp.int32)
    return keep_flags.reshape(RELAY_SECTIONS, TOKENS)


def levels(stream_key, dims, pieces, low, largest):
    level, own = 1.0, jax.random.fold_in(stream_key, 6)
    for dim, shards_of in pieces:
        heights = jnp.exp(jax.random.uniform(jax.random.fold_in(own, dim), (shards_of,), jnp.float32, low / len(pieces), largest / len(pieces)))
        level = level * jnp.repeat(heights, dims[dim] // shards_of).reshape([-1 if axis == dim else 1 for axis in range(len(dims))])
    return level


def scatter_about(stream_key, dims, width, most, cuts=(), kind=jnp.bfloat16):
    result = width * jax.random.normal(stream_key, dims, jnp.float32)
    if cuts:
        result = result * levels(stream_key, dims, cuts, -0.22, 0.18)
    return jnp.clip(result, -most, most).astype(kind)


def setup_inputs(seed: int = 0) -> dict:
    keys = jax.random.split(jax.random.key(seed), 7)
    out_cotangent = scatter_about(keys[0], (RELAY_SECTIONS, TOKENS, D), 1.0, 6.0, ((0, 16), (1, 32), (2, 2)))
    block_output = scatter_about(keys[1], (RELAY_SECTIONS, TOKENS, D), 1.0, 6.0, ((0, 16), (1, 32), (2, 2)))
    router_logits = scatter_about(keys[2], (RELAY_SECTIONS, TOKENS), 2.0, 8.0, ((0, 16), (1, 32)), jnp.float32)
    keep_flags = draw_keep_flags(jax.random.fold_in(keys[6], 71), 0)
    router_weight = scatter_about(keys[4], (RELAY_SECTIONS, D), D ** -0.5, 0.09375, ((0, 16), (1, 2)), jnp.float32)
    activated = scatter_about(keys[5], (RELAY_SECTIONS, GROUP_ACTIVE, HID), 0.25, 4.0, ((0, 16), (2, 32)))
    return {"out_cotangent": out_cotangent, "block_output": block_output, "router_logits": router_logits, "keep_flags": keep_flags, "router_weight": router_weight, "activated": activated}


def segment_part(cotangent, output, keep_row, logits, router_row, stored):
    dy_float = cotangent.astype(jnp.float32)
    gate_value = jax.nn.sigmoid(logits)
    grad_gate = jnp.sum(dy_float * output.astype(jnp.float32), axis=1)
    grad_score = keep_row.astype(jnp.float32) * grad_gate * gate_value * (1.0 - gate_value)
    dx_tokens = (dy_float + grad_score[:, None] * router_row[None, :]).astype(jnp.bfloat16)
    order = jnp.argsort(1 - keep_row, stable=True)[:GROUP_ACTIVE].astype(jnp.int32)
    dz_rows = (jnp.take(gate_value, order)[:, None] * jnp.take(dy_float, order, axis=0)).astype(jnp.bfloat16)
    gradient = jnp.dot(dz_rows.T, stored, preferred_element_type=jnp.float32).astype(jnp.bfloat16)
    return dx_tokens, gradient


def reference(out_cotangent, block_output, router_logits, keep_flags, router_weight, activated):
    def apply_segment(members):
        return segment_part(members[0], members[1], members[2], members[3], members[4], members[5])

    dx_all, grad_out = lax.map(apply_segment, (out_cotangent, block_output, keep_flags, router_logits, router_weight, activated))
    received = jnp.concatenate([dx_all[1:], jnp.zeros_like(dx_all[:1])], axis=0)
    return received, grad_out
```

```python
import functools

import jax
import jax.numpy as jnp
from jax import lax
from jax.experimental import pallas as pl
from jax.experimental.pallas import tpu as pltpu
from jax.sharding import PartitionSpec as P

MESH = pl.DeviceIdType.MESH
NX, NY = 4, 8
GROUP = NX * NY
HALF = 24
DEAD = 64.0
ROWS_A = 16
WIDTH = 64
ACTIVE = 512


def ring_plan():
    size = {"A": ROWS_A * 1024, "B": (WIDTH - ROWS_A) * 1024}
    first = {"A": "x", "B": "y"}
    second = {"A": "y", "B": "x"}
    length = {"x": NX, "y": NY}
    rate, latency = 46.6e3, 2.2

    messages = {}
    for c in "AB":
        n = length[first[c]]
        for s in (1, -1):
            for d in range(1, n // 2 + 1):
                messages[(c, 1, 0, s, d)] = size[c] * (0.5 if d == n // 2 else 1.0)
        m = length[second[c]]
        for e in range(n):
            for s in (1, -1):
                for d in range(1, m // 2 + 1):
                    messages[(c, 2, e, s, d)] = size[c] * (0.5 if d == m // 2 else 1.0)

    def needs(key):
        c, stage, e, s, d = key
        if d > 1:
            return [(c, stage, e, s, d - 1)]
        if stage == 1 or e == 0:
            return []
        n = length[first[c]]
        if e < n // 2:
            return [(c, 1, 0, 1, e)]
        if e > n // 2:
            return [(c, 1, 0, -1, n - e)]
        return [(c, 1, 0, 1, n // 2), (c, 1, 0, -1, n // 2)]

    def axis(key):
        return (first if key[1] == 1 else second)[key[0]]

    def rank(key):
        c, stage, e, s, d = key
        return (stage, 0 if c == "B" else 1, -d)

    free = {(a, s): 0.0 for a in "xy" for s in (1, -1)}
    arrived, waiting = {}, {}
    pending = set(messages)
    order = []
    while pending:
        best = None
        for key in pending:
            if any(k not in arrived for k in needs(key)):
                continue
            ready = max([0.0] + [arrived[k] for k in needs(key)])
            start = max(ready, free[(axis(key), key[3])])
            item = (start, rank(key), key)
            if best is None or item < best:
                best = item
        start, _, key = best
        link = (axis(key), key[3])
        free[link] = start + messages[key] / rate
        arrived[key] = start + messages[key] / rate + latency
        order.append((start, key))
        pending.remove(key)
    steps = []
    done = set()
    for start, key in sorted(order, key=lambda item: item[0]):
        for k in needs(key):
            if k not in done:
                done.add(k)
                steps.append(("wait", k))
        steps.append(("send", key))
    tail = sorted((k for k in messages if k not in done), key=lambda k: arrived[k])
    steps += [("wait", k) for k in tail]
    return steps, {k: i for i, k in enumerate(sorted(messages))}, max(arrived.values())


def wrapped(value, n):
    return lax.rem(value + 2 * n, n)


def kernel(
    cot_hbm, out_hbm, logit_hbm, keep_hbm, router_hbm, act_hbm,
    received_ref, grad_ref,
    cot, other, logit, keep, router, act,
    sent, landed, rows, shifted, part, peer_part, score, next_score, next_router,
    local_sem, all_send, all_recv, ring_send, ring_recv, side_send, side_recv,
):
    segment = lax.axis_index("segment")
    tok = lax.axis_index("tok")
    half = lax.axis_index("mp")
    x, y = tok // NY, lax.rem(tok, NY)
    last = lax.axis_size("segment") - 1

    loads = []
    for i, (src, dst) in enumerate((
        (cot_hbm, cot), (keep_hbm, keep), (logit_hbm, logit),
        (out_hbm, other), (router_hbm, router), (act_hbm, act),
    )):
        copy = pltpu.make_async_copy(src, dst, local_sem.at[i])
        copy.start()
        loads.append(copy)

    barrier = pltpu.get_barrier_semaphore()

    def greet(p, carry):
        to = (segment, lax.rem(tok + p, GROUP), half)
        pl.semaphore_signal(barrier, inc=1, device_id=to, device_id_type=MESH)
        return carry

    lax.fori_loop(1, GROUP, greet, 0)
    pl.semaphore_signal(barrier, inc=1, device_id=(segment, tok, 1 - half), device_id_type=MESH)

    @pl.when(segment > 0)
    def _():
        pl.semaphore_signal(barrier, inc=1, device_id=(segment - 1, tok, half), device_id_type=MESH)

    @pl.when(segment < last)
    def _():
        pl.semaphore_signal(barrier, inc=1, device_id=(segment + 1, tok, half), device_id_type=MESH)

    for copy in loads[:3]:
        copy.wait()
    keep_row = keep[...].astype(jnp.float32)
    gate_row = jax.nn.sigmoid(logit[...])
    upper = (
        lax.broadcasted_iota(jnp.int32, (128, 128), 0) <= lax.broadcasted_iota(jnp.int32, (128, 128), 1)
    ).astype(jnp.bfloat16)
    keep_wide = jnp.broadcast_to(keep_row, (8, 128)).astype(jnp.bfloat16)
    place = jnp.dot(keep_wide, upper, preferred_element_type=jnp.float32)[0:1]
    count = jnp.dot(keep_wide, jnp.ones((128, 128), jnp.bfloat16), preferred_element_type=jnp.float32)[0:1]
    slot = lax.broadcasted_iota(jnp.int32, (2 * HALF, 128), 0).astype(jnp.float32)
    chosen = (jnp.broadcast_to(place, slot.shape) == slot + 1.0) & (jnp.broadcast_to(keep_row, slot.shape) > 0.5)
    chooser = chosen.astype(jnp.float32).astype(jnp.bfloat16)
    gate_slot = jnp.sum(jnp.where(chosen, jnp.broadcast_to(gate_row, slot.shape), 0.0), axis=1, keepdims=True)
    dead = slot >= jnp.broadcast_to(count, slot.shape)
    low = lax.broadcasted_iota(jnp.int32, (HALF, 128), 1) < WIDTH
    for k in range(16):
        picked = jnp.dot(chooser, cot[:, 128 * k : 128 * (k + 1)], preferred_element_type=jnp.float32)
        picked = jnp.where(dead, DEAD, picked * gate_slot)
        top, bottom = picked[:HALF], picked[HALF:]
        sent[2 * k] = jnp.where(low, top, pltpu.roll(bottom, WIDTH, 1)).astype(jnp.bfloat16)
        sent[2 * k + 1] = jnp.where(low, pltpu.roll(top, WIDTH, 1), bottom).astype(jnp.bfloat16)

    ends = (segment > 0).astype(jnp.int32) + (segment < last).astype(jnp.int32)
    pl.semaphore_wait(barrier, GROUP + ends)

    def to_peer(p):
        peer = lax.rem(tok + p, GROUP)
        return pltpu.make_async_remote_copy(
            src_ref=sent.at[peer], dst_ref=landed.at[tok], send_sem=all_send.at[p], recv_sem=all_recv.at[p],
            device_id=(segment, peer, half), device_id_type=MESH,
        )

    def from_peer(p):
        peer = lax.rem(tok + GROUP - p, GROUP)
        return pltpu.make_async_remote_copy(
            src_ref=sent.at[tok], dst_ref=landed.at[peer], send_sem=all_send.at[p], recv_sem=all_recv.at[p],
            device_id=(segment, peer, half), device_id_type=MESH,
        )

    def send_one(p, carry):
        to_peer(p).start()
        return carry

    lax.fori_loop(1, GROUP, send_one, 0)

    def previous(i, src, dst):
        return pltpu.make_async_remote_copy(
            src_ref=src, dst_ref=dst, send_sem=side_send.at[i], recv_sem=side_recv.at[i],
            device_id=(lax.rem(segment + last, last + 1), tok, half), device_id_type=MESH,
        )

    whole = previous(0, cot, shifted)
    loads[4].wait()
    weights = previous(1, router, next_router)

    @pl.when(segment > 0)
    def _():
        whole.start()
        weights.start()

    loads[3].wait()
    total = jnp.zeros((128, 128), jnp.float32)
    for k in range(16):
        cut = slice(128 * k, 128 * (k + 1))
        total += cot[:, cut].astype(jnp.float32) * other[:, cut].astype(jnp.float32)
    part[...] = jnp.broadcast_to(jnp.sum(total.T, axis=0, keepdims=True), (8, 128))
    landed[tok] = sent[tok]
    swap = pltpu.make_async_remote_copy(
        src_ref=part, dst_ref=peer_part, send_sem=side_send.at[3], recv_sem=side_recv.at[3],
        device_id=(segment, tok, 1 - half), device_id_type=MESH,
    )
    swap.start()
    swap.wait()
    grad_gate = part[0:1] + peer_part[0:1]
    score[...] = jnp.broadcast_to(keep_row * grad_gate * gate_row * (1.0 - gate_row), (8, 128))
    scores = previous(2, score, next_score)

    @pl.when(segment > 0)
    def _():
        scores.start()

    def recv_one(p, carry):
        from_peer(p).wait_recv()
        return carry

    lax.fori_loop(1, GROUP, recv_one, 0)

    got = landed[...].astype(jnp.float32)
    k24 = lax.broadcasted_iota(jnp.int32, (GROUP, HALF, 128), 1).astype(jnp.float32)
    live_top = jnp.broadcast_to(got[:, :, 0:1], got.shape) < 0.5 * DEAD
    live_bottom = jnp.broadcast_to(got[:, :, WIDTH : WIDTH + 1], got.shape) < 0.5 * DEAD
    counts = jnp.sum(live_top.astype(jnp.float32) + live_bottom.astype(jnp.float32), axis=1)
    below = (
        lax.broadcasted_iota(jnp.int32, (GROUP, GROUP), 1) < lax.broadcasted_iota(jnp.int32, (GROUP, GROUP), 0)
    ).astype(jnp.bfloat16)
    offset = jnp.dot(below, counts.astype(jnp.bfloat16), preferred_element_type=jnp.float32)
    offset = jnp.broadcast_to(offset.reshape(GROUP, 1, 128), got.shape)
    rank_top = jnp.where(live_top, offset + k24, -1.0).reshape(GROUP * HALF, 128)
    rank_bottom = jnp.where(live_bottom, offset + k24 + HALF, -1.0).reshape(GROUP * HALF, 128)
    lane = lax.broadcasted_iota(jnp.int32, (GROUP * HALF, 128), 1).astype(jnp.float32)
    flipped = got.reshape(GROUP * HALF, 128).T.astype(jnp.bfloat16)
    own = pl.multiple_of(tok * WIDTH, WIDTH)
    for t in range(ACTIVE // 128):
        pick_top = (rank_top == lane + 128.0 * t).astype(jnp.float32).astype(jnp.bfloat16)
        pick_bottom = (rank_bottom == lane + 128.0 * t).astype(jnp.float32).astype(jnp.bfloat16)
        tile = jnp.dot(flipped[:WIDTH], pick_top, preferred_element_type=jnp.float32)
        tile += jnp.dot(flipped[WIDTH:], pick_bottom, preferred_element_type=jnp.float32)
        rows[pl.ds(own, WIDTH), 128 * t : 128 * (t + 1)] = tile.astype(jnp.bfloat16)

    steps, index, _ = ring_plan()

    def block(key, held):
        c, stage, e, s, d = key
        n = {("A", 1): NX, ("A", 2): NY, ("B", 1): NY, ("B", 2): NX}[(c, stage)]
        back = s * (d - 1 + (1 if held else 0))
        along = (x if n == NX else y) - back
        if stage == 1:
            sx, sy = (along, y) if n == NX else (x, along)
        elif c == "A":
            sx, sy = x - e, along
        else:
            sx, sy = along, y - e
        source = wrapped(sx, NX) * NY + wrapped(sy, NY)
        start, size = (0, ROWS_A) if c == "A" else (ROWS_A, WIDTH - ROWS_A)
        at = pl.ds(pl.multiple_of(source * WIDTH + start, 16), size)
        if d < n // 2:
            return rows.at[at]
        return rows.at[at, pl.ds(0 if s == 1 else ACTIVE // 2, ACTIVE // 2)]

    def ring(key, held):
        c, stage, e, s, d = key
        on_x = (c == "A") == (stage == 1)
        if on_x:
            to = wrapped(x + s, NX) * NY + y
        else:
            to = x * NY + wrapped(y + s, NY)
        ref = block(key, held)
        return pltpu.make_async_remote_copy(
            src_ref=ref, dst_ref=ref, send_sem=ring_send.at[index[key]], recv_sem=ring_recv.at[index[key]],
            device_id=(segment, to, half), device_id_type=MESH,
        )

    for what, key in steps:
        if what == "send":
            ring(key, False).start()
        else:
            ring(key, True).wait_recv()

    loads[5].wait()

    def multiply(i, carry):
        at = pl.multiple_of(i * 256, 256)
        product = lax.dot_general(
            act[...], rows[pl.ds(at, 256), :], (((1,), (1,)), ((), ())), preferred_element_type=jnp.float32
        )
        grad_ref[:, pl.ds(at, 256)] = product.astype(jnp.bfloat16)
        return carry

    lax.fori_loop(0, 8, multiply, 0)

    @pl.when(segment < last)
    def _():
        whole.wait_recv()
        weights.wait_recv()
        scores.wait_recv()
        column = jnp.broadcast_to(next_score[0:1], (128, 128)).T
        for k in range(16):
            cut = slice(128 * k, 128 * (k + 1))
            row = jnp.broadcast_to(next_router[:, cut], (128, 128))
            received_ref[:, cut] = (shifted[:, cut].astype(jnp.float32) + column * row).astype(jnp.bfloat16)

    @pl.when(segment == last)
    def _():
        received_ref[...] = jnp.zeros_like(received_ref)

    @pl.when(segment > 0)
    def _():
        whole.wait_send()
        weights.wait_send()
        scores.wait_send()

    def sent_one(p, carry):
        to_peer(p).wait_send()
        return carry

    lax.fori_loop(1, GROUP, sent_one, 0)
    for what, key in steps:
        if what == "send":
            ring(key, False).wait_send()


def per_device(out_cotangent, block_output, router_logits, keep_flags, router_weight, activated):
    anywhere = pl.BlockSpec(memory_space=pltpu.HBM)
    inside = pl.BlockSpec(memory_space=pltpu.VMEM)
    messages = len(ring_plan()[1])
    bf16, f32 = jnp.bfloat16, jnp.float32
    received, gradient = pl.pallas_call(
        kernel,
        out_shape=(jax.ShapeDtypeStruct((128, 2048), bf16), jax.ShapeDtypeStruct((448, 2048), bf16)),
        in_specs=[anywhere] * 6,
        out_specs=(inside, inside),
        scratch_shapes=[
            pltpu.VMEM((128, 2048), bf16),
            pltpu.VMEM((128, 2048), bf16),
            pltpu.VMEM((1, 128), f32),
            pltpu.VMEM((1, 128), jnp.int32),
            pltpu.VMEM((1, 2048), f32),
            pltpu.VMEM((448, 512), bf16),
            pltpu.VMEM((GROUP, HALF, 128), bf16),
            pltpu.VMEM((GROUP, HALF, 128), bf16),
            pltpu.VMEM((GROUP * WIDTH, ACTIVE), bf16),
            pltpu.VMEM((128, 2048), bf16),
            pltpu.VMEM((8, 128), f32),
            pltpu.VMEM((8, 128), f32),
            pltpu.VMEM((8, 128), f32),
            pltpu.VMEM((8, 128), f32),
            pltpu.VMEM((1, 2048), f32),
            pltpu.SemaphoreType.DMA((6,)),
            pltpu.SemaphoreType.DMA((GROUP,)),
            pltpu.SemaphoreType.DMA((GROUP,)),
            pltpu.SemaphoreType.DMA((messages,)),
            pltpu.SemaphoreType.DMA((messages,)),
            pltpu.SemaphoreType.DMA((4,)),
            pltpu.SemaphoreType.DMA((4,)),
        ],
        compiler_params=pltpu.CompilerParams(collective_id=0, has_side_effects=True, vmem_limit_bytes=48 << 20),
    )(
        out_cotangent[0], block_output[0], router_logits, keep_flags, router_weight, activated[0].T,
    )
    return received[None], gradient.T[None]


def solution(mesh):
    in_specs = (
        P("segment", "tok", "mp"),
        P("segment", "tok", "mp"),
        P("segment", "tok"),
        P("segment", "tok"),
        P("segment", "mp"),
        P("segment", None, "tok"),
    )
    out_specs = (P("segment", "tok", "mp"), P("segment", "mp", "tok"))
    return jax.shard_map(per_device, mesh=mesh, in_specs=in_specs, out_specs=out_specs, check_vma=False)
```

```python
import functools

import jax
import jax.numpy as jnp
from jax import lax
from jax.experimental import pallas as pl
from jax.experimental.pallas import tpu as pltpu
from jax.sharding import PartitionSpec as P

MESH = pl.DeviceIdType.MESH
NX, NY = 4, 8
GROUP = NX * NY
HALF = 24
DEAD = 64.0
ROWS_A = 24
WIDTH = 64
ACTIVE = 512


def ring_plan():
    size = {"A": ROWS_A * 1024, "B": (WIDTH - ROWS_A) * 1024}
    first = {"A": "x", "B": "y"}
    second = {"A": "y", "B": "x"}
    length = {"x": NX, "y": NY}
    rate, latency = 46.6e3, 1.9

    messages = {}
    for c in "AB":
        n = length[first[c]]
        for s in (1, -1):
            for d in range(1, n // 2 + 1):
                messages[(c, 1, 0, s, d)] = size[c] * (0.5 if d == n // 2 else 1.0)
        m = length[second[c]]
        for e in range(n):
            for s in (1, -1):
                for d in range(1, m // 2 + 1):
                    messages[(c, 2, e, s, d)] = size[c] * (0.5 if d == m // 2 else 1.0)

    def needs(key):
        c, stage, e, s, d = key
        if d > 1:
            return [(c, stage, e, s, d - 1)]
        if stage == 1 or e == 0:
            return []
        n = length[first[c]]
        if e < n // 2:
            return [(c, 1, 0, 1, e)]
        if e > n // 2:
            return [(c, 1, 0, -1, n - e)]
        return [(c, 1, 0, 1, n // 2), (c, 1, 0, -1, n // 2)]

    def axis(key):
        return (first if key[1] == 1 else second)[key[0]]

    after = {key: [] for key in messages}
    for key in messages:
        for k in needs(key):
            after[k].append(key)

    @functools.cache
    def depth(key):
        return messages[key] / rate + latency + max([depth(k) for k in after[key]], default=0.0)

    def rank(key):
        return -depth(key)

    free = {(a, s): 0.0 for a in "xy" for s in (1, -1)}
    arrived, waiting = {}, {}
    pending = set(messages)
    order = []
    while pending:
        best = None
        for key in pending:
            if any(k not in arrived for k in needs(key)):
                continue
            ready = max([0.0] + [arrived[k] for k in needs(key)])
            start = max(ready, free[(axis(key), key[3])])
            item = (start, rank(key), key)
            if best is None or item < best:
                best = item
        start, _, key = best
        link = (axis(key), key[3])
        free[link] = start + messages[key] / rate
        arrived[key] = start + messages[key] / rate + latency
        order.append((start, key))
        pending.remove(key)
    steps = []
    done = set()
    for start, key in sorted(order, key=lambda item: item[0]):
        for k in needs(key):
            if k not in done:
                done.add(k)
                steps.append(("wait", k))
        steps.append(("send", key))
    tail = sorted((k for k in messages if k not in done), key=lambda k: arrived[k])
    head = len(steps)
    steps += [("wait", k) for k in tail]
    return steps, head, {k: i for i, k in enumerate(sorted(messages))}, max(arrived.values())


def wrapped(value, n):
    return lax.rem(value + 2 * n, n)


def kernel(
    cot_hbm, out_hbm, logit_hbm, keep_hbm, router_hbm,
    received_ref, rows,
    cot, other, logit, keep, router,
    sent, landed, shifted, part, peer_part, score, next_score, next_router,
    local_sem, all_send, all_recv, ring_send, ring_recv, side_send, side_recv,
):
    segment = lax.axis_index("segment")
    tok = lax.axis_index("tok")
    half = lax.axis_index("mp")
    x, y = tok // NY, lax.rem(tok, NY)
    last = lax.axis_size("segment") - 1

    loads = []
    for i, (src, dst) in enumerate((
        (cot_hbm, cot), (keep_hbm, keep), (logit_hbm, logit),
        (out_hbm, other), (router_hbm, router),
    )):
        copy = pltpu.make_async_copy(src, dst, local_sem.at[i])
        copy.start()
        loads.append(copy)

    barrier = pltpu.get_barrier_semaphore()

    peers = sorted(
        ((dx, dy) for dx in range(NX) for dy in range(NY) if dx or dy),
        key=lambda at: -(min(at[0], NX - at[0]) + min(at[1], NY - at[1])),
    )

    def away(at, sign):
        return wrapped(x + sign * at[0], NX) * NY + wrapped(y + sign * at[1], NY)

    for at in peers:
        pl.semaphore_signal(barrier, inc=1, device_id=(segment, away(at, 1), half), device_id_type=MESH)

    @pl.when(segment < last)
    def _():
        pl.semaphore_signal(barrier, inc=1, device_id=(segment + 1, tok, half), device_id_type=MESH)

    @pl.when(half == 0)
    def _():
        pl.semaphore_signal(barrier, inc=1, device_id=(segment, tok, 1), device_id_type=MESH)

    for copy in loads[:3]:
        copy.wait()
    keep_row = keep[...].astype(jnp.float32)
    gate_row = jax.nn.sigmoid(logit[...])
    upper = (
        lax.broadcasted_iota(jnp.int32, (128, 128), 0) <= lax.broadcasted_iota(jnp.int32, (128, 128), 1)
    ).astype(jnp.bfloat16)
    keep_wide = jnp.broadcast_to(keep_row, (8, 128)).astype(jnp.bfloat16)
    place = jnp.dot(keep_wide, upper, preferred_element_type=jnp.float32)[0:1]
    count = jnp.dot(keep_wide, jnp.ones((128, 128), jnp.bfloat16), preferred_element_type=jnp.float32)[0:1]
    slot = lax.broadcasted_iota(jnp.int32, (2 * HALF, 128), 0).astype(jnp.float32)
    chosen = (jnp.broadcast_to(place, slot.shape) == slot + 1.0) & (jnp.broadcast_to(keep_row, slot.shape) > 0.5)
    chooser = chosen.astype(jnp.float32).astype(jnp.bfloat16)
    gate_slot = jnp.sum(jnp.where(chosen, jnp.broadcast_to(gate_row, slot.shape), 0.0), axis=1, keepdims=True)
    dead = slot >= jnp.broadcast_to(count, slot.shape)
    low = lax.broadcasted_iota(jnp.int32, (HALF, 128), 1) < WIDTH
    for k in range(16):
        picked = jnp.dot(chooser, cot[:, 128 * k : 128 * (k + 1)], preferred_element_type=jnp.float32)
        picked = jnp.where(dead, DEAD, picked * gate_slot)
        top, bottom = picked[:HALF], picked[HALF:]
        sent[2 * k] = jnp.where(low, top, pltpu.roll(bottom, WIDTH, 1)).astype(jnp.bfloat16)
        sent[2 * k + 1] = jnp.where(low, pltpu.roll(top, WIDTH, 1), bottom).astype(jnp.bfloat16)

    pl.semaphore_wait(barrier, GROUP - 1 + (segment > 0).astype(jnp.int32) + half)

    def exchange(at, sign):
        peer, i = away(at, sign), at[0] * NY + at[1]
        return pltpu.make_async_remote_copy(
            src_ref=sent.at[peer if sign > 0 else tok], dst_ref=landed.at[tok if sign > 0 else peer],
            send_sem=all_send.at[i], recv_sem=all_recv.at[i],
            device_id=(segment, peer, half), device_id_type=MESH,
        )

    for at in peers:
        exchange(at, 1).start()

    def previous(i, src, dst):
        return pltpu.make_async_remote_copy(
            src_ref=src, dst_ref=dst, send_sem=side_send.at[i], recv_sem=side_recv.at[i],
            device_id=(lax.rem(segment + last, last + 1), tok, half), device_id_type=MESH,
        )

    whole = previous(0, cot, shifted)
    loads[4].wait()
    weights = previous(1, router, next_router)

    @pl.when(segment > 0)
    def _():
        whole.start()
        weights.start()

    loads[3].wait()
    total = jnp.zeros((128, 128), jnp.float32)
    for k in range(16):
        cut = slice(128 * k, 128 * (k + 1))
        total += cot[:, cut].astype(jnp.float32) * other[:, cut].astype(jnp.float32)
    part[...] = jnp.broadcast_to(jnp.sum(total.T, axis=0, keepdims=True), (8, 128))
    landed[tok] = sent[tok]
    swap = pltpu.make_async_remote_copy(
        src_ref=part, dst_ref=peer_part, send_sem=side_send.at[3], recv_sem=side_recv.at[3],
        device_id=(segment, tok, 1 - half), device_id_type=MESH,
    )

    @pl.when(half == 1)
    def _():
        swap.start()

    scores = previous(2, score, next_score)

    def answer():
        @pl.when(half == 0)
        def _():
            swap.wait_recv()
            swap.start()

    def tell():
        @pl.when(half == 1)
        def _():
            swap.wait_recv()

        grad_gate = part[0:1] + peer_part[0:1]
        score[...] = jnp.broadcast_to(keep_row * grad_gate * gate_row * (1.0 - gate_row), (8, 128))

        @pl.when(segment > 0)
        def _():
            scores.start()

    for at in peers:
        exchange(at, -1).wait_recv()

    got = landed[...].astype(jnp.float32)
    k24 = lax.broadcasted_iota(jnp.int32, (GROUP, HALF, 128), 1).astype(jnp.float32)
    live_top = jnp.broadcast_to(got[:, :, 0:1], got.shape) < 0.5 * DEAD
    live_bottom = jnp.broadcast_to(got[:, :, WIDTH : WIDTH + 1], got.shape) < 0.5 * DEAD
    counts = jnp.sum(live_top.astype(jnp.float32) + live_bottom.astype(jnp.float32), axis=1)
    below = (
        lax.broadcasted_iota(jnp.int32, (GROUP, GROUP), 1) < lax.broadcasted_iota(jnp.int32, (GROUP, GROUP), 0)
    ).astype(jnp.bfloat16)
    offset = jnp.dot(below, counts.astype(jnp.bfloat16), preferred_element_type=jnp.float32)
    offset = jnp.broadcast_to(offset.reshape(GROUP, 1, 128), got.shape)
    rank_top = jnp.where(live_top, offset + k24, -1.0).reshape(GROUP * HALF, 128)
    rank_bottom = jnp.where(live_bottom, offset + k24 + HALF, -1.0).reshape(GROUP * HALF, 128)
    lane = lax.broadcasted_iota(jnp.int32, (GROUP * HALF, 128), 1).astype(jnp.float32)
    flipped = got.reshape(GROUP * HALF, 128).T.astype(jnp.bfloat16)
    own = pl.multiple_of(tok * WIDTH, WIDTH)
    for t in range(ACTIVE // 128):
        pick_top = (rank_top == lane + 128.0 * t).astype(jnp.float32).astype(jnp.bfloat16)
        pick_bottom = (rank_bottom == lane + 128.0 * t).astype(jnp.float32).astype(jnp.bfloat16)
        tile = jnp.dot(flipped[:WIDTH], pick_top, preferred_element_type=jnp.float32)
        tile += jnp.dot(flipped[WIDTH:], pick_bottom, preferred_element_type=jnp.float32)
        rows[pl.ds(own, WIDTH), 128 * t : 128 * (t + 1)] = tile.astype(jnp.bfloat16)

    steps, head, index, _ = ring_plan()

    def block(key, held):
        c, stage, e, s, d = key
        n = {("A", 1): NX, ("A", 2): NY, ("B", 1): NY, ("B", 2): NX}[(c, stage)]
        back = s * (d - 1 + (1 if held else 0))
        along = (x if n == NX else y) - back
        if stage == 1:
            sx, sy = (along, y) if n == NX else (x, along)
        elif c == "A":
            sx, sy = x - e, along
        else:
            sx, sy = along, y - e
        source = wrapped(sx, NX) * NY + wrapped(sy, NY)
        start, size = (0, ROWS_A) if c == "A" else (ROWS_A, WIDTH - ROWS_A)
        at = pl.ds(pl.multiple_of(source * WIDTH + start, 8), size)
        if d < n // 2:
            return rows.at[at]
        return rows.at[at, pl.ds(0 if s == 1 else ACTIVE // 2, ACTIVE // 2)]

    def ring(key, held):
        c, stage, e, s, d = key
        on_x = (c == "A") == (stage == 1)
        if on_x:
            to = wrapped(x + s, NX) * NY + y
        else:
            to = x * NY + wrapped(y + s, NY)
        ref = block(key, held)
        return pltpu.make_async_remote_copy(
            src_ref=ref, dst_ref=ref, send_sem=ring_send.at[index[key]], recv_sem=ring_recv.at[index[key]],
            device_id=(segment, to, half), device_id_type=MESH,
        )

    def receive():
        @pl.when(segment < last)
        def _():
            whole.wait_recv()
            weights.wait_recv()
            scores.wait_recv()
            column = jnp.broadcast_to(next_score[0:1], (128, 128)).T
            for k in range(16):
                cut = slice(128 * k, 128 * (k + 1))
                row = jnp.broadcast_to(next_router[:, cut], (128, 128))
                received_ref[:, cut] = (shifted[:, cut].astype(jnp.float32) + column * row).astype(jnp.bfloat16)

        @pl.when(segment == last)
        def _():
            received_ref[...] = jnp.zeros_like(received_ref)

    for i, (what, key) in enumerate(steps):
        if i == head // 4:
            answer()
        if i == head // 2:
            tell()
        if i == head:
            receive()
        if what == "send":
            ring(key, False).start()
        else:
            ring(key, True).wait_recv()

    @pl.when(segment > 0)
    def _():
        whole.wait_send()
        weights.wait_send()
        scores.wait_send()

    swap.wait_send()
    for at in peers:
        exchange(at, 1).wait_send()
    for what, key in steps:
        if what == "send":
            ring(key, False).wait_send()


def finish(received_ref, rows, act, received_hbm, grad_hbm, grad, sems):
    first = pltpu.make_async_copy(received_ref, received_hbm, sems.at[8])
    first.start()
    copies = [first]
    for i in range(8):
        cut = slice(256 * i, 256 * (i + 1))
        product = lax.dot_general(
            act[...], rows[cut, :], (((1,), (1,)), ((), ())), preferred_element_type=jnp.float32
        )
        grad[i] = product.astype(jnp.bfloat16)
        copy = pltpu.make_async_copy(grad.at[i], grad_hbm.at[:, cut], sems.at[i])
        copy.start()
        copies.append(copy)
    for copy in copies:
        copy.wait()


def per_device(out_cotangent, block_output, router_logits, keep_flags, router_weight, activated):
    anywhere = pl.BlockSpec(memory_space=pltpu.HBM)
    inside = pl.BlockSpec(memory_space=pltpu.VMEM)
    messages = len(ring_plan()[2])
    bf16, f32 = jnp.bfloat16, jnp.float32
    far = [
        pltpu.with_memory_space_constraint(a, pltpu.HBM)
        for a in (out_cotangent[0], block_output[0], router_logits, keep_flags, router_weight)
    ]
    received, rows = pl.pallas_call(
        kernel,
        out_shape=(jax.ShapeDtypeStruct((128, 2048), bf16), jax.ShapeDtypeStruct((GROUP * WIDTH, ACTIVE), bf16)),
        in_specs=[anywhere] * 5,
        out_specs=(inside, inside),
        scratch_shapes=[
            pltpu.VMEM((128, 2048), bf16),
            pltpu.VMEM((128, 2048), bf16),
            pltpu.VMEM((1, 128), f32),
            pltpu.VMEM((1, 128), jnp.int32),
            pltpu.VMEM((1, 2048), f32),
            pltpu.VMEM((GROUP, HALF, 128), bf16),
            pltpu.VMEM((GROUP, HALF, 128), bf16),
            pltpu.VMEM((128, 2048), bf16),
            pltpu.VMEM((8, 128), f32),
            pltpu.VMEM((8, 128), f32),
            pltpu.VMEM((8, 128), f32),
            pltpu.VMEM((8, 128), f32),
            pltpu.VMEM((1, 2048), f32),
            pltpu.SemaphoreType.DMA((5,)),
            pltpu.SemaphoreType.DMA((GROUP,)),
            pltpu.SemaphoreType.DMA((GROUP,)),
            pltpu.SemaphoreType.DMA((messages,)),
            pltpu.SemaphoreType.DMA((messages,)),
            pltpu.SemaphoreType.DMA((4,)),
            pltpu.SemaphoreType.DMA((4,)),
        ],
        compiler_params=pltpu.CompilerParams(collective_id=0, has_side_effects=True, vmem_limit_bytes=48 << 20),
        cost_estimate=pl.CostEstimate(flops=20_000_000_000, bytes_accessed=2 << 20, transcendentals=0),
    )(*far)
    received, gradient = pl.pallas_call(
        finish,
        out_shape=(jax.ShapeDtypeStruct((128, 2048), bf16), jax.ShapeDtypeStruct((448, 2048), bf16)),
        in_specs=[inside] * 3,
        out_specs=(anywhere, anywhere),
        scratch_shapes=[pltpu.VMEM((8, 448, 256), bf16), pltpu.SemaphoreType.DMA((9,))],
        compiler_params=pltpu.CompilerParams(vmem_limit_bytes=48 << 20),
        cost_estimate=pl.CostEstimate(flops=1_000_000_000, bytes_accessed=5 << 20, transcendentals=0),
    )(received, rows, activated[0].T)
    return received[None], gradient.T[None]


def solution(mesh):
    in_specs = (
        P("segment", "tok", "mp"),
        P("segment", "tok", "mp"),
        P("segment", "tok"),
        P("segment", "tok"),
        P("segment", "mp"),
        P("segment", None, "tok"),
    )
    out_specs = (P("segment", "tok", "mp"), P("segment", "mp", "tok"))
    return jax.shard_map(per_device, mesh=mesh, in_specs=in_specs, out_specs=out_specs, check_vma=False)
```

```python
import functools

import jax
import jax.numpy as jnp
from jax import lax
from jax.experimental import pallas as pl
from jax.experimental.pallas import tpu as pltpu
from jax.sharding import PartitionSpec as P

MESH = pl.DeviceIdType.MESH
NX, NY = 4, 8
GROUP = NX * NY
HALF = 24
DEAD = 64.0
ROWS_A = 24
WIDTH = 64
ACTIVE = 512


SPLIT = {"A": 2, "B": 2}
PARENT = {
    ("A", 1): {1: 0, 2: 1},
    ("A", 2): {1: 0, 2: 1, 3: 2, 4: 2},
    ("B", 1): {1: 0, 2: 0, 3: 2, 4: 2},
    ("B", 2): {1: 0, 2: 1},
}


@functools.cache
def ring_plan():
    rate, latency, hop = 46.6e3, 2.6, 0.75
    size = {"A": ROWS_A * 1024 / SPLIT["A"], "B": (WIDTH - ROWS_A) * 1024 / SPLIT["B"]}
    messages, needs = {}, {}
    for c in "AB":
        n, m = (NX, NY) if c == "A" else (NY, NX)
        for u in range(SPLIT[c]):
            for stage, ring, offsets in ((1, n, (0,)), (2, m, range(n))):
                for e in offsets:
                    if stage == 1 or e == 0:
                        base = []
                    elif e < n // 2:
                        base = [(c, u, 1, 0, 1, e)]
                    elif e > n // 2:
                        base = [(c, u, 1, 0, -1, n - e)]
                    else:
                        base = [(c, u, 1, 0, 1, e), (c, u, 1, 0, -1, e)]
                    for s in (1, -1):
                        for d in range(1, ring // 2 + 1):
                            key, parent = (c, u, stage, e, s, d), PARENT[c, stage][d]
                            messages[key] = (size[c] * (0.5 if d == ring // 2 else 1.0), d - parent)
                            needs[key] = [(c, u, stage, e, s, parent)] if parent else base
    after = {key: [] for key in messages}
    for key in messages:
        for k in needs[key]:
            after[k].append(key)

    @functools.cache
    def depth(key):
        nbytes, hops = messages[key]
        own = nbytes * hops / rate + latency + hop * (hops - 1)
        return own + max([depth(k) for k in after[key]], default=0.0)

    def link(key):
        return ((key[0] == "A") == (key[2] == 1), key[4])

    free, arrived, order = {}, {}, []
    pending = set(messages)
    while pending:
        best = None
        for key in pending:
            if all(k in arrived for k in needs[key]):
                ready = max([0.0] + [arrived[k] for k in needs[key]])
                item = (max(ready, free.get(link(key), 0.0)), -depth(key), key)
                best = item if best is None else min(best, item)
        start, _, key = best
        nbytes, hops = messages[key]
        free[link(key)] = start + nbytes * hops / rate
        arrived[key] = free[link(key)] + latency + hop * (hops - 1)
        order.append((start, key))
        pending.remove(key)
    steps, done = [], set()
    for start, key in sorted(order, key=lambda item: item[0]):
        for k in needs[key]:
            if k not in done:
                done.add(k)
                steps.append(("wait", k))
        steps.append(("send", key))
    head = len(steps)
    steps += [("wait", k) for k in sorted((k for k in messages if k not in done), key=lambda k: arrived[k])]
    return steps, head, {k: i for i, k in enumerate(sorted(messages))}, max(arrived.values())


def wrapped(value, n):
    return lax.rem(value + 2 * n, n)


def kernel(
    cot_hbm, out_hbm, logit_hbm, keep_hbm, router_hbm,
    received_ref, rows,
    cot, other, logit, keep, router,
    sent, landed, shifted, part, peer_part, score, next_score, next_router,
    local_sem, all_send, all_recv, ring_send, ring_recv, side_send, side_recv, first_ready, shift_ready,
):
    segment = lax.axis_index("segment")
    tok = lax.axis_index("tok")
    half = lax.axis_index("mp")
    x, y = tok // NY, lax.rem(tok, NY)
    last = lax.axis_size("segment") - 1

    loads = []
    for i, (src, dst) in enumerate((
        (cot_hbm, cot), (keep_hbm, keep), (logit_hbm, logit),
        (out_hbm, other), (router_hbm, router),
    )):
        copy = pltpu.make_async_copy(src, dst, local_sem.at[i])
        copy.start()
        loads.append(copy)

    barrier = pltpu.get_barrier_semaphore()

    peers = sorted(
        ((dx, dy) for dx in range(NX) for dy in range(NY) if dx or dy),
        key=lambda at: -(min(at[0], NX - at[0]) + min(at[1], NY - at[1])),
    )

    def away(at, sign):
        return wrapped(x + sign * at[0], NX) * NY + wrapped(y + sign * at[1], NY)

    others = tok != 0

    @pl.when(others)
    def _():
        for at in peers:
            pl.semaphore_signal(barrier, inc=1, device_id=(segment, away(at, 1), half), device_id_type=MESH)

    @pl.when(others & (segment < last))
    def _():
        pl.semaphore_signal(barrier, inc=1, device_id=(segment + 1, tok, half), device_id_type=MESH)

    @pl.when((tok == 0) & (segment > 0))
    def _():
        pl.semaphore_signal(barrier, inc=1, device_id=(segment - 1, tok, half), device_id_type=MESH)

    @pl.when(half == 0)
    def _():
        pl.semaphore_signal(barrier, inc=1, device_id=(segment, tok, 1), device_id_type=MESH)

    beside = jnp.where(others, (segment > 0).astype(jnp.int32), (segment < last).astype(jnp.int32))
    entered = GROUP - 1 - others.astype(jnp.int32) + beside + half

    @pl.when(tok == 0)
    def _():
        pl.semaphore_wait(barrier, entered)
        for at in peers:
            pl.semaphore_signal(first_ready, inc=1, device_id=(segment, away(at, 1), half), device_id_type=MESH)

    @pl.when((tok == 0) & (segment < last))
    def _():
        pl.semaphore_signal(shift_ready, inc=1, device_id=(segment + 1, tok, half), device_id_type=MESH)

    for copy in loads[:3]:
        copy.wait()
    keep_row = keep[...].astype(jnp.float32)
    gate_row = jax.nn.sigmoid(logit[...])
    upper = (
        lax.broadcasted_iota(jnp.int32, (128, 128), 0) <= lax.broadcasted_iota(jnp.int32, (128, 128), 1)
    ).astype(jnp.bfloat16)
    keep_wide = jnp.broadcast_to(keep_row, (8, 128)).astype(jnp.bfloat16)
    place = jnp.dot(keep_wide, upper, preferred_element_type=jnp.float32)[0:1]
    count = jnp.dot(keep_wide, jnp.ones((128, 128), jnp.bfloat16), preferred_element_type=jnp.float32)[0:1]
    slot = lax.broadcasted_iota(jnp.int32, (2 * HALF, 128), 0).astype(jnp.float32)
    chosen = (jnp.broadcast_to(place, slot.shape) == slot + 1.0) & (jnp.broadcast_to(keep_row, slot.shape) > 0.5)
    chooser = chosen.astype(jnp.float32).astype(jnp.bfloat16)
    gate_slot = jnp.sum(jnp.where(chosen, jnp.broadcast_to(gate_row, slot.shape), 0.0), axis=1, keepdims=True)
    dead = slot >= jnp.broadcast_to(count, slot.shape)
    low = lax.broadcasted_iota(jnp.int32, (HALF, 128), 1) < WIDTH
    for k in range(16):
        picked = jnp.dot(chooser, cot[:, 128 * k : 128 * (k + 1)], preferred_element_type=jnp.float32)
        picked = jnp.where(dead, DEAD, picked * gate_slot)
        top, bottom = picked[:HALF], picked[HALF:]
        sent[2 * k] = jnp.where(low, top, pltpu.roll(bottom, WIDTH, 1)).astype(jnp.bfloat16)
        sent[2 * k + 1] = jnp.where(low, pltpu.roll(top, WIDTH, 1), bottom).astype(jnp.bfloat16)

    @pl.when(others)
    def _():
        pl.semaphore_wait(barrier, entered)

    def exchange(at, sign):
        peer = away(at, sign)
        return pltpu.make_async_remote_copy(
            src_ref=sent.at[peer if sign > 0 else tok], dst_ref=landed.at[tok if sign > 0 else peer],
            send_sem=all_send, recv_sem=all_recv,
            device_id=(segment, peer, half), device_id_type=MESH,
        )

    for at in peers:

        @pl.when(away(at, 1) != 0)
        def _():
            exchange(at, 1).start()

    def previous(i, src, dst):
        return pltpu.make_async_remote_copy(
            src_ref=src, dst_ref=dst, send_sem=side_send.at[i], recv_sem=side_recv.at[i],
            device_id=(lax.rem(segment + last, last + 1), tok, half), device_id_type=MESH,
        )

    whole = previous(0, cot, shifted)
    loads[4].wait()
    weights = previous(1, router, next_router)

    @pl.when(others & (segment > 0))
    def _():
        whole.start()
        weights.start()

    def late_shift():
        @pl.when((tok == 0) & (segment > 0))
        def _():
            pl.semaphore_wait(shift_ready, 1)
            whole.start()
            weights.start()

    loads[3].wait()
    total = jnp.zeros((128, 128), jnp.float32)
    for k in range(16):
        cut = slice(128 * k, 128 * (k + 1))
        total += cot[:, cut].astype(jnp.float32) * other[:, cut].astype(jnp.float32)
    part[...] = jnp.broadcast_to(jnp.sum(total.T, axis=0, keepdims=True), (8, 128))
    landed[tok] = sent[tok]
    swap = pltpu.make_async_remote_copy(
        src_ref=part, dst_ref=peer_part, send_sem=side_send.at[3], recv_sem=side_recv.at[3],
        device_id=(segment, tok, 1 - half), device_id_type=MESH,
    )

    @pl.when(half == 1)
    def _():
        swap.start()

    scores = previous(2, score, next_score)

    def answer():
        @pl.when(half == 0)
        def _():
            swap.wait_recv()
            swap.start()

    def tell():
        @pl.when(half == 1)
        def _():
            swap.wait_recv()

        grad_gate = part[0:1] + peer_part[0:1]
        score[...] = jnp.broadcast_to(keep_row * grad_gate * gate_row * (1.0 - gate_row), (8, 128))

        @pl.when(segment > 0)
        def _():
            scores.start()

    @pl.when(others)
    def _():
        pl.semaphore_wait(first_ready, 1)
        pltpu.make_async_remote_copy(
            src_ref=sent.at[0], dst_ref=landed.at[tok], send_sem=all_send, recv_sem=all_recv,
            device_id=(segment, 0, half), device_id_type=MESH,
        ).start()

    every = pltpu.make_async_remote_copy(
        src_ref=sent.at[pl.ds(0, GROUP - 1)], dst_ref=landed.at[pl.ds(0, GROUP - 1)],
        send_sem=all_send, recv_sem=all_recv,
        device_id=(segment, away((0, 1), 1), half), device_id_type=MESH,
    )
    every.wait_recv()

    got = landed[...].astype(jnp.float32)
    k24 = lax.broadcasted_iota(jnp.int32, (GROUP, HALF, 128), 1).astype(jnp.float32)
    live_top = jnp.broadcast_to(got[:, :, 0:1], got.shape) < 0.5 * DEAD
    live_bottom = jnp.broadcast_to(got[:, :, WIDTH : WIDTH + 1], got.shape) < 0.5 * DEAD
    counts = jnp.sum(live_top.astype(jnp.float32) + live_bottom.astype(jnp.float32), axis=1)
    below = (
        lax.broadcasted_iota(jnp.int32, (GROUP, GROUP), 1) < lax.broadcasted_iota(jnp.int32, (GROUP, GROUP), 0)
    ).astype(jnp.bfloat16)
    offset = jnp.dot(below, counts.astype(jnp.bfloat16), preferred_element_type=jnp.float32)
    offset = jnp.broadcast_to(offset.reshape(GROUP, 1, 128), got.shape)
    rank_top = jnp.where(live_top, offset + k24, -1.0).reshape(GROUP * HALF, 128)
    rank_bottom = jnp.where(live_bottom, offset + k24 + HALF, -1.0).reshape(GROUP * HALF, 128)
    lane = lax.broadcasted_iota(jnp.int32, (GROUP * HALF, 128), 1).astype(jnp.float32)
    flipped = got.reshape(GROUP * HALF, 128).T.astype(jnp.bfloat16)
    own = pl.multiple_of(tok * WIDTH, WIDTH)
    for t in range(ACTIVE // 128):
        pick_top = (rank_top == lane + 128.0 * t).astype(jnp.float32).astype(jnp.bfloat16)
        pick_bottom = (rank_bottom == lane + 128.0 * t).astype(jnp.float32).astype(jnp.bfloat16)
        tile = jnp.dot(flipped[:WIDTH], pick_top, preferred_element_type=jnp.float32)
        tile += jnp.dot(flipped[WIDTH:], pick_bottom, preferred_element_type=jnp.float32)
        rows[pl.ds(own, WIDTH), 128 * t : 128 * (t + 1)] = tile.astype(jnp.bfloat16)

    steps, head, index, _ = ring_plan()

    def block(key, held):
        c, u, stage, e, s, d = key
        on_x = (c == "A") == (stage == 1)
        along = (x if on_x else y) - s * (d if held else PARENT[c, stage][d])
        if stage == 1:
            sx, sy = (along, y) if on_x else (x, along)
        else:
            sx, sy = (along, y - e) if on_x else (x - e, along)
        source = wrapped(sx, NX) * NY + wrapped(sy, NY)
        start, size = (0, ROWS_A) if c == "A" else (ROWS_A, WIDTH - ROWS_A)
        at = pl.ds(pl.multiple_of(source * WIDTH + start, 8), size)
        lanes = ACTIVE // SPLIT[c]
        first = lanes * u
        if d == (NX if on_x else NY) // 2:
            lanes //= 2
            first += 0 if s == 1 else lanes
        return rows.at[at, pl.ds(first, lanes)]

    def ring(key, held):
        c, u, stage, e, s, d = key
        step = s * (d - PARENT[c, stage][d])
        if (c == "A") == (stage == 1):
            to = wrapped(x + step, NX) * NY + y
        else:
            to = x * NY + wrapped(y + step, NY)
        ref = block(key, held)
        return pltpu.make_async_remote_copy(
            src_ref=ref, dst_ref=ref, send_sem=ring_send, recv_sem=ring_recv.at[index[key]],
            device_id=(segment, to, half), device_id_type=MESH,
        )

    def receive():
        @pl.when(segment < last)
        def _():
            whole.wait_recv()
            weights.wait_recv()
            scores.wait_recv()
            column = jnp.broadcast_to(next_score[0:1], (128, 128)).T
            for k in range(16):
                cut = slice(128 * k, 128 * (k + 1))
                row = jnp.broadcast_to(next_router[:, cut], (128, 128))
                received_ref[:, cut] = (shifted[:, cut].astype(jnp.float32) + column * row).astype(jnp.bfloat16)

        @pl.when(segment == last)
        def _():
            received_ref[...] = jnp.zeros_like(received_ref)

    for i, (what, key) in enumerate(steps):
        if i == 12:
            late_shift()
        if i == head // 4:
            answer()
        if i == head // 2:
            tell()
        if i == head:
            receive()
        if what == "send":
            ring(key, False).start()
        else:
            ring(key, True).wait_recv()

    @pl.when(segment > 0)
    def _():
        whole.wait_send()
        weights.wait_send()
        scores.wait_send()

    swap.wait_send()
    every.wait_send()
    gone = rows.at[pl.ds(0, (GROUP - 1) * WIDTH)]
    pltpu.make_async_remote_copy(
        src_ref=gone, dst_ref=gone, send_sem=ring_send, recv_sem=ring_recv.at[0],
        device_id=(segment, away((0, 1), 1), half), device_id_type=MESH,
    ).wait_send()


def finish(received_ref, rows, act, received_hbm, grad_hbm, grad, sems):
    first = pltpu.make_async_copy(received_ref, received_hbm, sems.at[8])
    first.start()
    copies = [first]
    for i in range(8):
        cut = slice(256 * i, 256 * (i + 1))
        product = lax.dot_general(
            act[...], rows[cut, :], (((1,), (1,)), ((), ())), preferred_element_type=jnp.float32
        )
        grad[i] = product.astype(jnp.bfloat16)
        copy = pltpu.make_async_copy(grad.at[i], grad_hbm.at[:, cut], sems.at[i])
        copy.start()
        copies.append(copy)
    for copy in copies:
        copy.wait()


def per_device(out_cotangent, block_output, router_logits, keep_flags, router_weight, activated):
    anywhere = pl.BlockSpec(memory_space=pltpu.HBM)
    inside = pl.BlockSpec(memory_space=pltpu.VMEM)
    messages = len(ring_plan()[2])
    bf16, f32 = jnp.bfloat16, jnp.float32
    far = [
        pltpu.with_memory_space_constraint(a, pltpu.HBM)
        for a in (out_cotangent[0], block_output[0], router_logits, keep_flags, router_weight)
    ]
    received, rows = pl.pallas_call(
        kernel,
        out_shape=(jax.ShapeDtypeStruct((128, 2048), bf16), jax.ShapeDtypeStruct((GROUP * WIDTH, ACTIVE), bf16)),
        in_specs=[anywhere] * 5,
        out_specs=(inside, inside),
        scratch_shapes=[
            pltpu.VMEM((128, 2048), bf16),
            pltpu.VMEM((128, 2048), bf16),
            pltpu.VMEM((1, 128), f32),
            pltpu.VMEM((1, 128), jnp.int32),
            pltpu.VMEM((1, 2048), f32),
            pltpu.VMEM((GROUP, HALF, 128), bf16),
            pltpu.VMEM((GROUP, HALF, 128), bf16),
            pltpu.VMEM((128, 2048), bf16),
            pltpu.VMEM((8, 128), f32),
            pltpu.VMEM((8, 128), f32),
            pltpu.VMEM((8, 128), f32),
            pltpu.VMEM((8, 128), f32),
            pltpu.VMEM((1, 2048), f32),
            pltpu.SemaphoreType.DMA((5,)),
            pltpu.SemaphoreType.DMA,
            pltpu.SemaphoreType.DMA,
            pltpu.SemaphoreType.DMA,
            pltpu.SemaphoreType.DMA((messages,)),
            pltpu.SemaphoreType.DMA((4,)),
            pltpu.SemaphoreType.DMA((4,)),
            pltpu.SemaphoreType.REGULAR,
            pltpu.SemaphoreType.REGULAR,
        ],
        compiler_params=pltpu.CompilerParams(collective_id=0, has_side_effects=True, vmem_limit_bytes=48 << 20),
        cost_estimate=pl.CostEstimate(flops=20_000_000_000, bytes_accessed=2 << 20, transcendentals=0),
    )(*far)
    received, gradient = pl.pallas_call(
        finish,
        out_shape=(jax.ShapeDtypeStruct((128, 2048), bf16), jax.ShapeDtypeStruct((448, 2048), bf16)),
        in_specs=[inside] * 3,
        out_specs=(anywhere, anywhere),
        scratch_shapes=[pltpu.VMEM((8, 448, 256), bf16), pltpu.SemaphoreType.DMA((9,))],
        compiler_params=pltpu.CompilerParams(vmem_limit_bytes=48 << 20),
        cost_estimate=pl.CostEstimate(flops=1_000_000_000, bytes_accessed=5 << 20, transcendentals=0),
    )(received, rows, activated[0].T)
    return received[None], gradient.T[None]


def solution(mesh):
    in_specs = (
        P("segment", "tok", "mp"),
        P("segment", "tok", "mp"),
        P("segment", "tok"),
        P("segment", "tok"),
        P("segment", "mp"),
        P("segment", None, "tok"),
    )
    out_specs = (P("segment", "tok", "mp"), P("segment", "mp", "tok"))
    return jax.shard_map(per_device, mesh=mesh, in_specs=in_specs, out_specs=out_specs, check_vma=False)
```

```python
import functools

import jax
import jax.numpy as jnp
from jax import lax
from jax.experimental import pallas as pl
from jax.experimental.pallas import tpu as pltpu
from jax.sharding import PartitionSpec as P

MESH = pl.DeviceIdType.MESH
NX, NY = 4, 8
GROUP = NX * NY
HALF = 24
DEAD = 64.0
ROWS_A = 24
WIDTH = 64
ACTIVE = 512


LATE = 3.0
SPLIT = {"A": 2, "B": 2}
PARENT = {
    ("A", 1): {1: 0, 2: 1},
    ("A", 2): {1: 0, 2: 1, 3: 2, 4: 2},
    ("B", 1): {1: 0, 2: 0, 3: 2, 4: 2},
    ("B", 2): {1: 0, 2: 1},
}


@functools.cache
def ring_plan():
    rate, latency, hop = 46.6e3, 3.7, 0.75
    size = {"A": ROWS_A * 1024 / SPLIT["A"], "B": (WIDTH - ROWS_A) * 1024 / SPLIT["B"]}
    messages, needs = {}, {}
    for c in "AB":
        n, m = (NX, NY) if c == "A" else (NY, NX)
        for u in range(SPLIT[c]):
            for stage, ring, offsets in ((1, n, (0,)), (2, m, range(n))):
                for e in offsets:
                    if stage == 1 or e == 0:
                        base = []
                    elif e < n // 2:
                        base = [(c, u, 1, 0, 1, e)]
                    elif e > n // 2:
                        base = [(c, u, 1, 0, -1, n - e)]
                    else:
                        base = [(c, u, 1, 0, 1, e), (c, u, 1, 0, -1, e)]
                    for s in (1, -1):
                        for d in range(1, ring // 2 + 1):
                            key, parent = (c, u, stage, e, s, d), PARENT[c, stage][d]
                            messages[key] = (size[c] * (0.5 if d == ring // 2 else 1.0), d - parent)
                            needs[key] = [(c, u, stage, e, s, parent)] if parent else base
    after = {key: [] for key in messages}
    for key in messages:
        for k in needs[key]:
            after[k].append(key)

    @functools.cache
    def depth(key):
        nbytes, hops = messages[key]
        own = nbytes * hops / rate + latency + hop * (hops - 1)
        return own + max([depth(k) for k in after[key]], default=0.0)

    def link(key):
        return ((key[0] == "A") == (key[2] == 1), key[4])

    free, arrived, order = {}, {}, []
    pending = set(messages)
    while pending:
        best = None
        for key in pending:
            if all(k in arrived for k in needs[key]):
                ready = max([0.0] + [arrived[k] for k in needs[key]])
                item = (max(ready, free.get(link(key), 0.0)), -depth(key), key)
                best = item if best is None else min(best, item)
        start, _, key = best
        nbytes, hops = messages[key]
        free[link(key)] = start + nbytes * hops / rate
        arrived[key] = free[link(key)] + latency + hop * (hops - 1)
        order.append((start, key))
        pending.remove(key)
    items = []
    for late in (False, True):
        done = set()
        for start, key in sorted(order, key=lambda item: item[0]):
            fresh = tuple(k for k in needs[key] if k not in done)
            done.update(fresh)
            if needs[key]:
                items.append((start + (LATE if late else 0.0), late, fresh, key))
            elif not late:
                items.append((start, None, (), key))
    items.sort(key=lambda item: item[0])
    passed = [k for k in sorted(messages) if k in done]
    ends = [k for k in messages if k not in done]
    index = {k: i for i, k in enumerate(passed)} | {k: len(passed) for k in ends}
    return items, index, int(sum(messages[k][0] for k in ends)), max(arrived.values())


def wrapped(value, n):
    return lax.rem(value + 2 * n, n)


def kernel(
    cot_hbm, out_hbm, logit_hbm, keep_hbm, router_hbm,
    received_ref, rows,
    cot, other, logit, keep, router,
    sent, landed, shifted, part, peer_part, score, next_score, next_router,
    local_sem, all_send, all_recv, ring_send, ring_recv, side_send, side_recv, first_ready, shift_ready,
):
    segment = lax.axis_index("segment")
    tok = lax.axis_index("tok")
    half = lax.axis_index("mp")
    x, y = tok // NY, lax.rem(tok, NY)
    last = lax.axis_size("segment") - 1

    loads = []
    for i, (src, dst) in enumerate((
        (cot_hbm, cot), (keep_hbm, keep), (logit_hbm, logit),
        (out_hbm, other), (router_hbm, router),
    )):
        copy = pltpu.make_async_copy(src, dst, local_sem.at[i])
        copy.start()
        loads.append(copy)

    barrier = pltpu.get_barrier_semaphore()

    peers = sorted(
        ((dx, dy) for dx in range(NX) for dy in range(NY) if dx or dy),
        key=lambda at: -(min(at[0], NX - at[0]) + min(at[1], NY - at[1])),
    )

    def away(at, sign):
        return wrapped(x + sign * at[0], NX) * NY + wrapped(y + sign * at[1], NY)

    others = tok != 0

    @pl.when(others)
    def _():
        for at in peers:
            pl.semaphore_signal(barrier, inc=1, device_id=(segment, away(at, 1), half), device_id_type=MESH)

    @pl.when(others & (segment < last))
    def _():
        pl.semaphore_signal(barrier, inc=1, device_id=(segment + 1, tok, half), device_id_type=MESH)

    @pl.when((tok == 0) & (segment > 0))
    def _():
        pl.semaphore_signal(barrier, inc=1, device_id=(segment - 1, tok, half), device_id_type=MESH)

    @pl.when(half == 0)
    def _():
        pl.semaphore_signal(barrier, inc=1, device_id=(segment, tok, 1), device_id_type=MESH)

    beside = jnp.where(others, (segment > 0).astype(jnp.int32), (segment < last).astype(jnp.int32))
    entered = GROUP - 1 - others.astype(jnp.int32) + beside + half

    @pl.when(tok == 0)
    def _():
        pl.semaphore_wait(barrier, entered)
        for at in peers:
            pl.semaphore_signal(first_ready, inc=1, device_id=(segment, away(at, 1), half), device_id_type=MESH)

    @pl.when((tok == 0) & (segment < last))
    def _():
        pl.semaphore_signal(shift_ready, inc=1, device_id=(segment + 1, tok, half), device_id_type=MESH)

    for copy in loads[:3]:
        copy.wait()
    keep_row = keep[...].astype(jnp.float32)
    gate_row = jax.nn.sigmoid(logit[...])
    upper = (
        lax.broadcasted_iota(jnp.int32, (128, 128), 0) <= lax.broadcasted_iota(jnp.int32, (128, 128), 1)
    ).astype(jnp.bfloat16)
    keep_wide = jnp.broadcast_to(keep_row, (8, 128)).astype(jnp.bfloat16)
    place = jnp.dot(keep_wide, upper, preferred_element_type=jnp.float32)[0:1]
    count = jnp.dot(keep_wide, jnp.ones((128, 128), jnp.bfloat16), preferred_element_type=jnp.float32)[0:1]
    slot = lax.broadcasted_iota(jnp.int32, (2 * HALF, 128), 0).astype(jnp.float32)
    chosen = (jnp.broadcast_to(place, slot.shape) == slot + 1.0) & (jnp.broadcast_to(keep_row, slot.shape) > 0.5)
    chooser = chosen.astype(jnp.float32).astype(jnp.bfloat16)
    gate_slot = jnp.sum(jnp.where(chosen, jnp.broadcast_to(gate_row, slot.shape), 0.0), axis=1, keepdims=True)
    dead = slot >= jnp.broadcast_to(count, slot.shape)
    low = lax.broadcasted_iota(jnp.int32, (HALF, 128), 1) < WIDTH
    for k in range(16):
        picked = jnp.dot(chooser, cot[:, 128 * k : 128 * (k + 1)], preferred_element_type=jnp.float32)
        picked = jnp.where(dead, DEAD, picked * gate_slot)
        top, bottom = picked[:HALF], picked[HALF:]
        sent[2 * k] = jnp.where(low, top, pltpu.roll(bottom, WIDTH, 1)).astype(jnp.bfloat16)
        sent[2 * k + 1] = jnp.where(low, pltpu.roll(top, WIDTH, 1), bottom).astype(jnp.bfloat16)

    @pl.when(others)
    def _():
        pl.semaphore_wait(barrier, entered)

    def exchange(at, sign):
        peer = away(at, sign)
        return pltpu.make_async_remote_copy(
            src_ref=sent.at[peer if sign > 0 else tok], dst_ref=landed.at[tok if sign > 0 else peer],
            send_sem=all_send, recv_sem=all_recv,
            device_id=(segment, peer, half), device_id_type=MESH,
        )

    for at in peers:

        @pl.when(away(at, 1) != 0)
        def _():
            exchange(at, 1).start()

    def previous(i, src, dst):
        return pltpu.make_async_remote_copy(
            src_ref=src, dst_ref=dst, send_sem=side_send.at[i], recv_sem=side_recv.at[i],
            device_id=(lax.rem(segment + last, last + 1), tok, half), device_id_type=MESH,
        )

    whole = previous(0, cot, shifted)
    loads[4].wait()
    weights = previous(1, router, next_router)

    @pl.when(others & (segment > 0))
    def _():
        whole.start()
        weights.start()

    def late_shift():
        @pl.when((tok == 0) & (segment > 0))
        def _():
            pl.semaphore_wait(shift_ready, 1)
            whole.start()
            weights.start()

    loads[3].wait()
    total = jnp.zeros((128, 128), jnp.float32)
    for k in range(16):
        cut = slice(128 * k, 128 * (k + 1))
        total += cot[:, cut].astype(jnp.float32) * other[:, cut].astype(jnp.float32)
    part[...] = jnp.broadcast_to(jnp.sum(total.T, axis=0, keepdims=True), (8, 128))
    landed[tok] = sent[tok]
    swap = pltpu.make_async_remote_copy(
        src_ref=part, dst_ref=peer_part, send_sem=side_send.at[3], recv_sem=side_recv.at[3],
        device_id=(segment, tok, 1 - half), device_id_type=MESH,
    )

    @pl.when(half == 1)
    def _():
        swap.start()

    scores = previous(2, score, next_score)

    def answer():
        @pl.when(half == 0)
        def _():
            swap.wait_recv()
            swap.start()

    def tell():
        @pl.when(half == 1)
        def _():
            swap.wait_recv()

        grad_gate = part[0:1] + peer_part[0:1]
        score[...] = jnp.broadcast_to(keep_row * grad_gate * gate_row * (1.0 - gate_row), (8, 128))

        @pl.when(segment > 0)
        def _():
            scores.start()

    @pl.when(others)
    def _():
        pl.semaphore_wait(first_ready, 1)
        pltpu.make_async_remote_copy(
            src_ref=sent.at[0], dst_ref=landed.at[tok], send_sem=all_send, recv_sem=all_recv,
            device_id=(segment, 0, half), device_id_type=MESH,
        ).start()

    every = pltpu.make_async_remote_copy(
        src_ref=sent.at[pl.ds(0, GROUP - 1)], dst_ref=landed.at[pl.ds(0, GROUP - 1)],
        send_sem=all_send, recv_sem=all_recv,
        device_id=(segment, away((0, 1), 1), half), device_id_type=MESH,
    )
    every.wait_recv()

    got = landed[...].astype(jnp.float32)
    k24 = lax.broadcasted_iota(jnp.int32, (GROUP, HALF, 128), 1).astype(jnp.float32)
    live_top = jnp.broadcast_to(got[:, :, 0:1], got.shape) < 0.5 * DEAD
    live_bottom = jnp.broadcast_to(got[:, :, WIDTH : WIDTH + 1], got.shape) < 0.5 * DEAD
    counts = jnp.sum(live_top.astype(jnp.float32) + live_bottom.astype(jnp.float32), axis=1)
    below = (
        lax.broadcasted_iota(jnp.int32, (GROUP, GROUP), 1) < lax.broadcasted_iota(jnp.int32, (GROUP, GROUP), 0)
    ).astype(jnp.bfloat16)
    offset = jnp.dot(below, counts.astype(jnp.bfloat16), preferred_element_type=jnp.float32)
    offset = jnp.broadcast_to(offset.reshape(GROUP, 1, 128), got.shape)
    rank_top = jnp.where(live_top, offset + k24, -1.0).reshape(GROUP * HALF, 128)
    rank_bottom = jnp.where(live_bottom, offset + k24 + HALF, -1.0).reshape(GROUP * HALF, 128)
    lane = lax.broadcasted_iota(jnp.int32, (GROUP * HALF, 128), 1).astype(jnp.float32)
    flipped = got.reshape(GROUP * HALF, 128).T.astype(jnp.bfloat16)
    own = pl.multiple_of(tok * WIDTH, WIDTH)
    for t in range(ACTIVE // 128):
        pick_top = (rank_top == lane + 128.0 * t).astype(jnp.float32).astype(jnp.bfloat16)
        pick_bottom = (rank_bottom == lane + 128.0 * t).astype(jnp.float32).astype(jnp.bfloat16)
        tile = jnp.dot(flipped[:WIDTH], pick_top, preferred_element_type=jnp.float32)
        tile += jnp.dot(flipped[WIDTH:], pick_bottom, preferred_element_type=jnp.float32)
        rows[pl.ds(own, WIDTH), 128 * t : 128 * (t + 1)] = tile.astype(jnp.bfloat16)

    items, index, end_bytes, _ = ring_plan()

    def origin(key, held):
        c, u, stage, e, s, d = key
        on_x = (c == "A") == (stage == 1)
        along = (x if on_x else y) - s * (d if held else PARENT[c, stage][d])
        if stage == 1:
            sx, sy = (along, y) if on_x else (x, along)
        else:
            sx, sy = (along, y - e) if on_x else (x - e, along)
        return wrapped(sx, NX) * NY + wrapped(sy, NY)

    def block(key, held):
        c, u, stage, e, s, d = key
        on_x = (c == "A") == (stage == 1)
        source = origin(key, held)
        start, size = (0, ROWS_A) if c == "A" else (ROWS_A, WIDTH - ROWS_A)
        at = pl.ds(pl.multiple_of(source * WIDTH + start, 8), size)
        lanes = ACTIVE // SPLIT[c]
        first = lanes * u
        if d == (NX if on_x else NY) // 2:
            lanes //= 2
            first += 0 if s == 1 else lanes
        return rows.at[at, pl.ds(first, lanes)]

    def ring(key, held):
        c, u, stage, e, s, d = key
        step = s * (d - PARENT[c, stage][d])
        if (c == "A") == (stage == 1):
            to = wrapped(x + step, NX) * NY + y
        else:
            to = x * NY + wrapped(y + step, NY)
        ref = block(key, held)
        return pltpu.make_async_remote_copy(
            src_ref=ref, dst_ref=ref, send_sem=ring_send, recv_sem=ring_recv.at[index[key]],
            device_id=(segment, to, half), device_id_type=MESH,
        )

    def receive():
        @pl.when(segment < last)
        def _():
            whole.wait_recv()
            weights.wait_recv()
            scores.wait_recv()
            column = jnp.broadcast_to(next_score[0:1], (128, 128)).T
            for k in range(16):
                cut = slice(128 * k, 128 * (k + 1))
                row = jnp.broadcast_to(next_router[:, cut], (128, 128))
                received_ref[:, cut] = (shifted[:, cut].astype(jnp.float32) + column * row).astype(jnp.bfloat16)

        @pl.when(segment == last)
        def _():
            received_ref[...] = jnp.zeros_like(received_ref)

    extra = [(1.2, late_shift), (4.5, answer), (8.0, tell)]
    for when, late, waits, key in items:
        while extra and extra[0][0] <= when:
            extra.pop(0)[1]()
        if late is None:
            ring(key, False).start()
            continue
        source = origin(key, False)

        @pl.when(source == 0 if late else source != 0)
        def _():
            for k in waits:
                ring(k, True).wait_recv()
            ring(key, False).start()

    for _, act_now in extra:
        act_now()
    receive()
    came = rows.at[pl.ds(0, end_bytes // (2 * ACTIVE))]
    pltpu.make_async_remote_copy(
        src_ref=came, dst_ref=came, send_sem=ring_send, recv_sem=ring_recv.at[max(index.values())],
        device_id=(segment, away((0, 1), 1), half), device_id_type=MESH,
    ).wait_recv()

    @pl.when(segment > 0)
    def _():
        whole.wait_send()
        weights.wait_send()
        scores.wait_send()

    swap.wait_send()
    every.wait_send()
    gone = rows.at[pl.ds(0, (GROUP - 1) * WIDTH)]
    pltpu.make_async_remote_copy(
        src_ref=gone, dst_ref=gone, send_sem=ring_send, recv_sem=ring_recv.at[0],
        device_id=(segment, away((0, 1), 1), half), device_id_type=MESH,
    ).wait_send()


def finish(received_ref, rows, act, received_hbm, grad_hbm, grad, sems):
    first = pltpu.make_async_copy(received_ref, received_hbm, sems.at[8])
    first.start()
    copies = [first]
    for i in range(8):
        cut = slice(256 * i, 256 * (i + 1))
        product = lax.dot_general(
            act[...], rows[cut, :], (((1,), (1,)), ((), ())), preferred_element_type=jnp.float32
        )
        grad[i] = product.astype(jnp.bfloat16)
        copy = pltpu.make_async_copy(grad.at[i], grad_hbm.at[:, cut], sems.at[i])
        copy.start()
        copies.append(copy)
    for copy in copies:
        copy.wait()


def per_device(out_cotangent, block_output, router_logits, keep_flags, router_weight, activated):
    anywhere = pl.BlockSpec(memory_space=pltpu.HBM)
    inside = pl.BlockSpec(memory_space=pltpu.VMEM)
    messages = 1 + max(ring_plan()[1].values())
    bf16, f32 = jnp.bfloat16, jnp.float32
    far = [
        pltpu.with_memory_space_constraint(a, pltpu.HBM)
        for a in (out_cotangent[0], block_output[0], router_logits, keep_flags, router_weight)
    ]
    received, rows = pl.pallas_call(
        kernel,
        out_shape=(jax.ShapeDtypeStruct((128, 2048), bf16), jax.ShapeDtypeStruct((GROUP * WIDTH, ACTIVE), bf16)),
        in_specs=[anywhere] * 5,
        out_specs=(inside, inside),
        scratch_shapes=[
            pltpu.VMEM((128, 2048), bf16),
            pltpu.VMEM((128, 2048), bf16),
            pltpu.VMEM((1, 128), f32),
            pltpu.VMEM((1, 128), jnp.int32),
            pltpu.VMEM((1, 2048), f32),
            pltpu.VMEM((GROUP, HALF, 128), bf16),
            pltpu.VMEM((GROUP, HALF, 128), bf16),
            pltpu.VMEM((128, 2048), bf16),
            pltpu.VMEM((8, 128), f32),
            pltpu.VMEM((8, 128), f32),
            pltpu.VMEM((8, 128), f32),
            pltpu.VMEM((8, 128), f32),
            pltpu.VMEM((1, 2048), f32),
            pltpu.SemaphoreType.DMA((5,)),
            pltpu.SemaphoreType.DMA,
            pltpu.SemaphoreType.DMA,
            pltpu.SemaphoreType.DMA,
            pltpu.SemaphoreType.DMA((messages,)),
            pltpu.SemaphoreType.DMA((4,)),
            pltpu.SemaphoreType.DMA((4,)),
            pltpu.SemaphoreType.REGULAR,
            pltpu.SemaphoreType.REGULAR,
        ],
        compiler_params=pltpu.CompilerParams(collective_id=0, has_side_effects=True, vmem_limit_bytes=48 << 20),
        cost_estimate=pl.CostEstimate(flops=20_000_000_000, bytes_accessed=2 << 20, transcendentals=0),
    )(*far)
    received, gradient = pl.pallas_call(
        finish,
        out_shape=(jax.ShapeDtypeStruct((128, 2048), bf16), jax.ShapeDtypeStruct((448, 2048), bf16)),
        in_specs=[inside] * 3,
        out_specs=(anywhere, anywhere),
        scratch_shapes=[pltpu.VMEM((8, 448, 256), bf16), pltpu.SemaphoreType.DMA((9,))],
        compiler_params=pltpu.CompilerParams(vmem_limit_bytes=48 << 20),
        cost_estimate=pl.CostEstimate(flops=1_000_000_000, bytes_accessed=5 << 20, transcendentals=0),
    )(received, rows, activated[0].T)
    return received[None], gradient.T[None]


def solution(mesh):
    in_specs = (
        P("segment", "tok", "mp"),
        P("segment", "tok", "mp"),
        P("segment", "tok"),
        P("segment", "tok"),
        P("segment", "mp"),
        P("segment", None, "tok"),
    )
    out_specs = (P("segment", "tok", "mp"), P("segment", "mp", "tok"))
    return jax.shard_map(per_device, mesh=mesh, in_specs=in_specs, out_specs=out_specs, check_vma=False)
```

```python
import functools

import jax
import jax.numpy as jnp
from jax import lax
from jax.experimental import pallas as pl
from jax.experimental.pallas import tpu as pltpu
from jax.sharding import PartitionSpec as P

MESH = pl.DeviceIdType.MESH
NX, NY = 4, 8
GROUP = NX * NY
HALF = 24
DEAD = 64.0
ROWS_A = 24
WIDTH = 64
ACTIVE = 512


LATE = 3.0
SPLIT = {"A": 2, "B": 2}
PARENT = {
    ("A", 1): {1: 0, 2: 1},
    ("A", 2): {1: 0, 2: 1, 3: 2, 4: 2},
    ("B", 1): {1: 0, 2: 0, 3: 2, 4: 2},
    ("B", 2): {1: 0, 2: 1},
}


@functools.cache
def ring_plan():
    rate, latency, hop = 46.6e3, 3.7, 0.75
    size = {"A": ROWS_A * 1024 / SPLIT["A"], "B": (WIDTH - ROWS_A) * 1024 / SPLIT["B"]}
    messages, needs = {}, {}
    for c in "AB":
        n, m = (NX, NY) if c == "A" else (NY, NX)
        for u in range(SPLIT[c]):
            side = 1 - 2 * (u % 2)
            for stage, ring, offsets in ((1, n, (0,)), (2, m, range(n))):
                for e in offsets:
                    if stage == 1 or e == 0:
                        base = []
                    elif e < n // 2:
                        base = [(c, u, 1, 0, 1, e)]
                    elif e > n // 2:
                        base = [(c, u, 1, 0, -1, n - e)]
                    else:
                        base = [(c, u, 1, 0, side, e)]
                    for s in (1, -1):
                        for d in range(1, ring // 2 + (1 if s == side else 0)):
                            key, parent = (c, u, stage, e, s, d), PARENT[c, stage][d]
                            messages[key] = (size[c], d - parent)
                            needs[key] = [(c, u, stage, e, s, parent)] if parent else base
    after = {key: [] for key in messages}
    for key in messages:
        for k in needs[key]:
            after[k].append(key)

    @functools.cache
    def depth(key):
        nbytes, hops = messages[key]
        own = nbytes * hops / rate + latency + hop * (hops - 1)
        return own + max([depth(k) for k in after[key]], default=0.0)

    def link(key):
        return ((key[0] == "A") == (key[2] == 1), key[4])

    free, arrived, order = {}, {}, []
    pending = set(messages)
    while pending:
        best = None
        for key in pending:
            if all(k in arrived for k in needs[key]):
                ready = max([0.0] + [arrived[k] for k in needs[key]])
                item = (max(ready, free.get(link(key), 0.0)), -depth(key), key)
                best = item if best is None else min(best, item)
        start, _, key = best
        nbytes, hops = messages[key]
        free[link(key)] = start + nbytes * hops / rate
        arrived[key] = free[link(key)] + latency + hop * (hops - 1)
        order.append((start, key))
        pending.remove(key)
    items = []
    for late in (False, True):
        done = set()
        for start, key in sorted(order, key=lambda item: item[0]):
            fresh = tuple(k for k in needs[key] if k not in done)
            done.update(fresh)
            if needs[key]:
                items.append((start + (LATE if late else 0.0), late, fresh, key))
            elif not late:
                items.append((start, None, (), key))
    items.sort(key=lambda item: item[0])
    passed = [k for k in sorted(messages) if k in done]
    ends = [k for k in messages if k not in done]
    index = {k: i for i, k in enumerate(passed)} | {k: len(passed) for k in ends}
    return items, index, int(sum(messages[k][0] for k in ends)), max(arrived.values())


def wrapped(value, n):
    return lax.rem(value + 2 * n, n)


def kernel(
    cot_hbm, out_hbm, logit_hbm, keep_hbm, router_hbm,
    received_ref, rows,
    cot, other, logit, keep, router,
    sent, landed, shifted, part, peer_part, score, next_score, next_router,
    local_sem, all_send, all_recv, ring_send, ring_recv, side_send, side_recv, first_ready, shift_ready,
):
    segment = lax.axis_index("segment")
    tok = lax.axis_index("tok")
    half = lax.axis_index("mp")
    x, y = tok // NY, lax.rem(tok, NY)
    last = lax.axis_size("segment") - 1

    loads = []
    for i, (src, dst) in enumerate((
        (cot_hbm, cot), (keep_hbm, keep), (logit_hbm, logit),
        (out_hbm, other), (router_hbm, router),
    )):
        copy = pltpu.make_async_copy(src, dst, local_sem.at[i])
        copy.start()
        loads.append(copy)

    barrier = pltpu.get_barrier_semaphore()

    peers = sorted(
        ((dx, dy) for dx in range(NX) for dy in range(NY) if dx or dy),
        key=lambda at: -(min(at[0], NX - at[0]) + min(at[1], NY - at[1])),
    )

    def away(at, sign):
        return wrapped(x + sign * at[0], NX) * NY + wrapped(y + sign * at[1], NY)

    others = tok != 0

    @pl.when(others)
    def _():
        for at in peers:
            pl.semaphore_signal(barrier, inc=1, device_id=(segment, away(at, 1), half), device_id_type=MESH)

    @pl.when(others & (segment < last))
    def _():
        pl.semaphore_signal(barrier, inc=1, device_id=(segment + 1, tok, half), device_id_type=MESH)

    @pl.when((tok == 0) & (segment > 0))
    def _():
        pl.semaphore_signal(barrier, inc=1, device_id=(segment - 1, tok, half), device_id_type=MESH)

    @pl.when(half == 0)
    def _():
        pl.semaphore_signal(barrier, inc=1, device_id=(segment, tok, 1), device_id_type=MESH)

    beside = jnp.where(others, (segment > 0).astype(jnp.int32), (segment < last).astype(jnp.int32))
    entered = GROUP - 1 - others.astype(jnp.int32) + beside + half

    @pl.when(tok == 0)
    def _():
        pl.semaphore_wait(barrier, entered)
        for at in peers:
            pl.semaphore_signal(first_ready, inc=1, device_id=(segment, away(at, 1), half), device_id_type=MESH)

    @pl.when((tok == 0) & (segment < last))
    def _():
        pl.semaphore_signal(shift_ready, inc=1, device_id=(segment + 1, tok, half), device_id_type=MESH)

    for copy in loads[:3]:
        copy.wait()
    keep_row = keep[...].astype(jnp.float32)
    gate_row = jax.nn.sigmoid(logit[...])
    upper = (
        lax.broadcasted_iota(jnp.int32, (128, 128), 0) <= lax.broadcasted_iota(jnp.int32, (128, 128), 1)
    ).astype(jnp.bfloat16)
    keep_wide = jnp.broadcast_to(keep_row, (8, 128)).astype(jnp.bfloat16)
    place = jnp.dot(keep_wide, upper, preferred_element_type=jnp.float32)[0:1]
    count = jnp.dot(keep_wide, jnp.ones((128, 128), jnp.bfloat16), preferred_element_type=jnp.float32)[0:1]
    slot = lax.broadcasted_iota(jnp.int32, (2 * HALF, 128), 0).astype(jnp.float32)
    chosen = (jnp.broadcast_to(place, slot.shape) == slot + 1.0) & (jnp.broadcast_to(keep_row, slot.shape) > 0.5)
    chooser = chosen.astype(jnp.float32).astype(jnp.bfloat16)
    gate_slot = jnp.sum(jnp.where(chosen, jnp.broadcast_to(gate_row, slot.shape), 0.0), axis=1, keepdims=True)
    dead = slot >= jnp.broadcast_to(count, slot.shape)
    low = lax.broadcasted_iota(jnp.int32, (HALF, 128), 1) < WIDTH
    for k in range(16):
        picked = jnp.dot(chooser, cot[:, 128 * k : 128 * (k + 1)], preferred_element_type=jnp.float32)
        picked = jnp.where(dead, DEAD, picked * gate_slot)
        top, bottom = picked[:HALF], picked[HALF:]
        sent[2 * k] = jnp.where(low, top, pltpu.roll(bottom, WIDTH, 1)).astype(jnp.bfloat16)
        sent[2 * k + 1] = jnp.where(low, pltpu.roll(top, WIDTH, 1), bottom).astype(jnp.bfloat16)

    @pl.when(others)
    def _():
        pl.semaphore_wait(barrier, entered)

    def exchange(at, sign):
        peer = away(at, sign)
        return pltpu.make_async_remote_copy(
            src_ref=sent.at[peer if sign > 0 else tok], dst_ref=landed.at[tok if sign > 0 else peer],
            send_sem=all_send, recv_sem=all_recv,
            device_id=(segment, peer, half), device_id_type=MESH,
        )

    for at in peers:

        @pl.when(away(at, 1) != 0)
        def _():
            exchange(at, 1).start()

    def previous(i, src, dst):
        return pltpu.make_async_remote_copy(
            src_ref=src, dst_ref=dst, send_sem=side_send.at[i], recv_sem=side_recv.at[i],
            device_id=(lax.rem(segment + last, last + 1), tok, half), device_id_type=MESH,
        )

    whole = previous(0, cot, shifted)
    loads[4].wait()
    weights = previous(1, router, next_router)

    @pl.when(others & (segment > 0))
    def _():
        whole.start()
        weights.start()

    def late_shift():
        @pl.when((tok == 0) & (segment > 0))
        def _():
            pl.semaphore_wait(shift_ready, 1)
            whole.start()
            weights.start()

    loads[3].wait()
    total = jnp.zeros((128, 128), jnp.float32)
    for k in range(16):
        cut = slice(128 * k, 128 * (k + 1))
        total += cot[:, cut].astype(jnp.float32) * other[:, cut].astype(jnp.float32)
    part[...] = jnp.broadcast_to(jnp.sum(total.T, axis=0, keepdims=True), (8, 128))
    landed[tok] = sent[tok]
    swap = pltpu.make_async_remote_copy(
        src_ref=part, dst_ref=peer_part, send_sem=side_send.at[3], recv_sem=side_recv.at[3],
        device_id=(segment, tok, 1 - half), device_id_type=MESH,
    )

    @pl.when(half == 1)
    def _():
        swap.start()

    scores = previous(2, score, next_score)

    def answer():
        @pl.when(half == 0)
        def _():
            swap.wait_recv()
            swap.start()

    def tell():
        @pl.when(half == 1)
        def _():
            swap.wait_recv()

        grad_gate = part[0:1] + peer_part[0:1]
        score[...] = jnp.broadcast_to(keep_row * grad_gate * gate_row * (1.0 - gate_row), (8, 128))

        @pl.when(segment > 0)
        def _():
            scores.start()

    @pl.when(others)
    def _():
        pl.semaphore_wait(first_ready, 1)
        pltpu.make_async_remote_copy(
            src_ref=sent.at[0], dst_ref=landed.at[tok], send_sem=all_send, recv_sem=all_recv,
            device_id=(segment, 0, half), device_id_type=MESH,
        ).start()

    every = pltpu.make_async_remote_copy(
        src_ref=sent.at[pl.ds(0, GROUP - 1)], dst_ref=landed.at[pl.ds(0, GROUP - 1)],
        send_sem=all_send, recv_sem=all_recv,
        device_id=(segment, away((0, 1), 1), half), device_id_type=MESH,
    )
    every.wait_recv()

    got = landed[...].astype(jnp.float32)
    k24 = lax.broadcasted_iota(jnp.int32, (GROUP, HALF, 128), 1).astype(jnp.float32)
    live_top = jnp.broadcast_to(got[:, :, 0:1], got.shape) < 0.5 * DEAD
    live_bottom = jnp.broadcast_to(got[:, :, WIDTH : WIDTH + 1], got.shape) < 0.5 * DEAD
    counts = jnp.sum(live_top.astype(jnp.float32) + live_bottom.astype(jnp.float32), axis=1)
    below = (
        lax.broadcasted_iota(jnp.int32, (GROUP, GROUP), 1) < lax.broadcasted_iota(jnp.int32, (GROUP, GROUP), 0)
    ).astype(jnp.bfloat16)
    offset = jnp.dot(below, counts.astype(jnp.bfloat16), preferred_element_type=jnp.float32)
    offset = jnp.broadcast_to(offset.reshape(GROUP, 1, 128), got.shape)
    rank_top = jnp.where(live_top, offset + k24, -1.0).reshape(GROUP * HALF, 128)
    rank_bottom = jnp.where(live_bottom, offset + k24 + HALF, -1.0).reshape(GROUP * HALF, 128)
    lane = lax.broadcasted_iota(jnp.int32, (GROUP * HALF, 128), 1).astype(jnp.float32)
    flipped = got.reshape(GROUP * HALF, 128).T.astype(jnp.bfloat16)
    own = pl.multiple_of(tok * WIDTH, WIDTH)
    for t in range(ACTIVE // 128):
        pick_top = (rank_top == lane + 128.0 * t).astype(jnp.float32).astype(jnp.bfloat16)
        pick_bottom = (rank_bottom == lane + 128.0 * t).astype(jnp.float32).astype(jnp.bfloat16)
        tile = jnp.dot(flipped[:WIDTH], pick_top, preferred_element_type=jnp.float32)
        tile += jnp.dot(flipped[WIDTH:], pick_bottom, preferred_element_type=jnp.float32)
        rows[pl.ds(own, WIDTH), 128 * t : 128 * (t + 1)] = tile.astype(jnp.bfloat16)

    items, index, end_bytes, _ = ring_plan()

    def origin(key, held):
        c, u, stage, e, s, d = key
        on_x = (c == "A") == (stage == 1)
        along = (x if on_x else y) - s * (d if held else PARENT[c, stage][d])
        if stage == 1:
            sx, sy = (along, y) if on_x else (x, along)
        else:
            sx, sy = (along, y - e) if on_x else (x - e, along)
        return wrapped(sx, NX) * NY + wrapped(sy, NY)

    def block(key, held):
        c, u, stage, e, s, d = key
        source = origin(key, held)
        start, size = (0, ROWS_A) if c == "A" else (ROWS_A, WIDTH - ROWS_A)
        at = pl.ds(pl.multiple_of(source * WIDTH + start, 8), size)
        lanes = ACTIVE // SPLIT[c]
        return rows.at[at, pl.ds(lanes * u, lanes)]

    def ring(key, held):
        c, u, stage, e, s, d = key
        step = s * (d - PARENT[c, stage][d])
        if (c == "A") == (stage == 1):
            to = wrapped(x + step, NX) * NY + y
        else:
            to = x * NY + wrapped(y + step, NY)
        ref = block(key, held)
        return pltpu.make_async_remote_copy(
            src_ref=ref, dst_ref=ref, send_sem=ring_send, recv_sem=ring_recv.at[index[key]],
            device_id=(segment, to, half), device_id_type=MESH,
        )

    def receive():
        @pl.when(segment < last)
        def _():
            whole.wait_recv()
            weights.wait_recv()
            scores.wait_recv()
            column = jnp.broadcast_to(next_score[0:1], (128, 128)).T
            for k in range(16):
                cut = slice(128 * k, 128 * (k + 1))
                row = jnp.broadcast_to(next_router[:, cut], (128, 128))
                received_ref[:, cut] = (shifted[:, cut].astype(jnp.float32) + column * row).astype(jnp.bfloat16)

        @pl.when(segment == last)
        def _():
            received_ref[...] = jnp.zeros_like(received_ref)

    extra = [(1.2, late_shift), (4.5, answer), (8.0, tell)]
    for when, late, waits, key in items:
        while extra and extra[0][0] <= when:
            extra.pop(0)[1]()
        if late is None:
            ring(key, False).start()
            continue
        source = origin(key, False)

        @pl.when(source == 0 if late else source != 0)
        def _():
            for k in waits:
                ring(k, True).wait_recv()
            ring(key, False).start()

    for _, act_now in extra:
        act_now()
    receive()
    came = rows.at[pl.ds(0, end_bytes // (2 * ACTIVE))]
    pltpu.make_async_remote_copy(
        src_ref=came, dst_ref=came, send_sem=ring_send, recv_sem=ring_recv.at[max(index.values())],
        device_id=(segment, away((0, 1), 1), half), device_id_type=MESH,
    ).wait_recv()

    @pl.when(segment > 0)
    def _():
        whole.wait_send()
        weights.wait_send()
        scores.wait_send()

    swap.wait_send()
    every.wait_send()
    gone = rows.at[pl.ds(0, (GROUP - 1) * WIDTH)]
    pltpu.make_async_remote_copy(
        src_ref=gone, dst_ref=gone, send_sem=ring_send, recv_sem=ring_recv.at[0],
        device_id=(segment, away((0, 1), 1), half), device_id_type=MESH,
    ).wait_send()


def finish(received_ref, rows, act, received_hbm, grad_hbm, grad, sems):
    first = pltpu.make_async_copy(received_ref, received_hbm, sems.at[8])
    first.start()
    copies = [first]
    for i in range(8):
        cut = slice(256 * i, 256 * (i + 1))
        product = lax.dot_general(
            act[...], rows[cut, :], (((1,), (1,)), ((), ())), preferred_element_type=jnp.float32
        )
        grad[i] = product.astype(jnp.bfloat16)
        copy = pltpu.make_async_copy(grad.at[i], grad_hbm.at[:, cut], sems.at[i])
        copy.start()
        copies.append(copy)
    for copy in copies:
        copy.wait()


def per_device(out_cotangent, block_output, router_logits, keep_flags, router_weight, activated):
    anywhere = pl.BlockSpec(memory_space=pltpu.HBM)
    inside = pl.BlockSpec(memory_space=pltpu.VMEM)
    messages = 1 + max(ring_plan()[1].values())
    bf16, f32 = jnp.bfloat16, jnp.float32
    far = [
        pltpu.with_memory_space_constraint(a, pltpu.HBM)
        for a in (out_cotangent[0], block_output[0], router_logits, keep_flags, router_weight)
    ]
    received, rows = pl.pallas_call(
        kernel,
        out_shape=(jax.ShapeDtypeStruct((128, 2048), bf16), jax.ShapeDtypeStruct((GROUP * WIDTH, ACTIVE), bf16)),
        in_specs=[anywhere] * 5,
        out_specs=(inside, inside),
        scratch_shapes=[
            pltpu.VMEM((128, 2048), bf16),
            pltpu.VMEM((128, 2048), bf16),
            pltpu.VMEM((1, 128), f32),
            pltpu.VMEM((1, 128), jnp.int32),
            pltpu.VMEM((1, 2048), f32),
            pltpu.VMEM((GROUP, HALF, 128), bf16),
            pltpu.VMEM((GROUP, HALF, 128), bf16),
            pltpu.VMEM((128, 2048), bf16),
            pltpu.VMEM((8, 128), f32),
            pltpu.VMEM((8, 128), f32),
            pltpu.VMEM((8, 128), f32),
            pltpu.VMEM((8, 128), f32),
            pltpu.VMEM((1, 2048), f32),
            pltpu.SemaphoreType.DMA((5,)),
            pltpu.SemaphoreType.DMA,
            pltpu.SemaphoreType.DMA,
            pltpu.SemaphoreType.DMA,
            pltpu.SemaphoreType.DMA((messages,)),
            pltpu.SemaphoreType.DMA((4,)),
            pltpu.SemaphoreType.DMA((4,)),
            pltpu.SemaphoreType.REGULAR,
            pltpu.SemaphoreType.REGULAR,
        ],
        compiler_params=pltpu.CompilerParams(collective_id=0, has_side_effects=True, vmem_limit_bytes=48 << 20),
        cost_estimate=pl.CostEstimate(flops=20_000_000_000, bytes_accessed=2 << 20, transcendentals=0),
    )(*far)
    received, gradient = pl.pallas_call(
        finish,
        out_shape=(jax.ShapeDtypeStruct((128, 2048), bf16), jax.ShapeDtypeStruct((448, 2048), bf16)),
        in_specs=[inside] * 3,
        out_specs=(anywhere, anywhere),
        scratch_shapes=[pltpu.VMEM((8, 448, 256), bf16), pltpu.SemaphoreType.DMA((9,))],
        compiler_params=pltpu.CompilerParams(vmem_limit_bytes=48 << 20),
        cost_estimate=pl.CostEstimate(flops=1_000_000_000, bytes_accessed=5 << 20, transcendentals=0),
    )(received, rows, activated[0].T)
    return received[None], gradient.T[None]


def solution(mesh):
    in_specs = (
        P("segment", "tok", "mp"),
        P("segment", "tok", "mp"),
        P("segment", "tok"),
        P("segment", "tok"),
        P("segment", "mp"),
        P("segment", None, "tok"),
    )
    out_specs = (P("segment", "tok", "mp"), P("segment", "mp", "tok"))
    return jax.shard_map(per_device, mesh=mesh, in_specs=in_specs, out_specs=out_specs, check_vma=False)
```
